768 devices in a mesh: gx: 16 (over y, x_hi), gy: 4 (over x_lo, core), gz: 12 (over z).
Axes of the slice: x: 4 (x_hi: 2, x_lo: 2; x = x_hi * 2 + x_lo), y: 8, z: 12, core: 2. Of those that a mesh axis runs over, the one named last changes fastest.
Arguments:
- rhs: float32 [3, 128, 64, 1536], P(None, 'gx', 'gy', 'gz'), may hold values from -24 to 24
- conductivity: float32 [8], replicated, may hold values from 0.1 to 10
- fraction: float32 [3, 128, 64, 1536], P(None, 'gx', 'gy', 'gz'), may hold values from 0.5 to 2
- region: int32 [128, 64, 1536], P('gx', 'gy', 'gz'), may hold values from 0 to 7
- flags: int32 [3, 128, 64, 1536], P(None, 'gx', 'gy', 'gz'), may hold values 0 or 1
Outputs:
- preconditioned: float32 [3, 128, 64, 1536], P(None, 'gx', 'gy', 'gz')
The draws below stay inside these ranges and needn't reach their ends.
All inputs are finite; a program needn't handle non-finite values. No bound on the sum of `flags` on one device may be relied on, other than what follows from the above.
Results may differ from the reference program's by a relative error of at most 0.00002.
Values sent between devices are 32-bit elements; how exact they have to be, the bound alone decides.
No kernel may reach another device: no remote copies, remote signals or barrier semaphores. Data moves between devices by JAX's collectives and lax.ppermute only.
A program may use at most 32 MiB of HBM per device.

```python
import math
import jax
import jax.numpy as jnp

REGIONS = 8
NX = 128
NY = 64
NZ = 1536


def place_ends(values, stream_key, low, largest):
    shape = values.shape
    spot = [jax.random.randint(jax.random.fold_in(stream_key, axis), (), 0, shape[axis]) for axis in range(len(shape))]
    values = values.at[tuple(spot)].set(low)
    longest = shape.index(max(shape))
    spot[longest] = (spot[longest] + 1) % shape[longest]
    return values.at[tuple(spot)].set(largest)


def shard_levels(key, extent, split, low, high):
    def one(dim, blocks):
        heights = jax.random.uniform(jax.random.fold_in(jax.random.fold_in(key, 6), dim), (blocks,), jnp.float32, low / len(split), high / len(split))
        return jnp.repeat(jnp.exp(heights), extent[dim] // blocks).reshape((-1,) + (1,) * (len(extent) - dim - 1))

    loudness = one(*split[0])
    for cut in split[1:]:
        loudness = loudness * one(*cut)
    return loudness


def scatter_about(rng, dims, width, limit, shards=(), kind=jnp.bfloat16):
    loudness = shard_levels(rng, dims, shards, -0.22, 0.18) if shards else 1.0
    values = jax.random.normal(rng, dims, jnp.float32) * width * loudness
    return jnp.minimum(jnp.maximum(values, -limit), limit).astype(kind)


def setup_inputs(seed: int = 0) -> dict:
    arg_keys = jax.random.split(jax.random.key(seed), 6)
    rhs = scatter_about(arg_keys[0], (3, NX, NY, NZ), 4.0, 24.0, ((1, 16), (2, 4), (3, 12)), jnp.float32)
    conductivity = jnp.clip(jnp.exp(jax.random.uniform(arg_keys[1], (REGIONS,), jnp.float32, math.log(0.1), math.log(10.0))), 0.1, 10.0)
    fraction = jnp.clip(jnp.exp(math.log(2.0) - 1.3862944 * jax.random.uniform(arg_keys[2], (3, NX, NY, NZ), jnp.float32) ** shard_levels(arg_keys[2], (3, NX, NY, NZ), ((1, 16), (2, 4), (3, 12)), -0.2, 0.2)), 0.5, 2.0)
    region = place_ends(jax.random.randint(arg_keys[3], (NX, NY, NZ), 0, REGIONS), jax.random.fold_in(arg_keys[3], 1), 0, REGIONS - 1).astype(jnp.int32)
    flags = place_ends((jax.random.randint(arg_keys[4], (3, NX, NY, NZ), 0, 8) < 1).astype(jnp.int32), jax.random.fold_in(arg_keys[4], 1), 0, 1)
    return dict(rhs=rhs, conductivity=conductivity, fraction=fraction, region=region, flags=flags)


edge_damping = 0.8
node_damping = 0.8


def upward(field, spatial):
    return jnp.roll(field, -1, axis=spatial)


def downward(field, spatial):
    return jnp.roll(field, 1, axis=spatial)


def forward_diff(field, spatial):
    return upward(field, spatial) - field


def backward_adjoint(field, spatial):
    return downward(field, spatial) - field


def curl_curl(stacked):
    first, second, third = stacked[0], stacked[1], stacked[2]
    face_zero = forward_diff(third, 1) - forward_diff(second, 2)
    face_one = forward_diff(first, 2) - forward_diff(third, 0)
    face_two = forward_diff(second, 0) - forward_diff(first, 1)
    return jnp.stack([backward_adjoint(face_one, 2) - backward_adjoint(face_two, 1),
                      backward_adjoint(face_two, 0) - backward_adjoint(face_zero, 2),
                      backward_adjoint(face_zero, 1) - backward_adjoint(face_one, 0)])


def conductance(conductivity, region):
    total = jnp.zeros(region.shape, conductivity.dtype)
    for number in range(conductivity.shape[0]):
        total = total + jnp.where(region == number, conductivity[number], jnp.zeros((), conductivity.dtype))
    return total


def masked_operator(field, keeping, sigma):
    masked = keeping * field
    return keeping * (curl_curl(masked) + sigma * masked) + (1.0 - keeping) * field


def nodal_operator(stacked):
    result = 7.0 * stacked
    for spatial in range(3):
        result = result - (jnp.roll(stacked, -1, axis=spatial + 1) + jnp.roll(stacked, 1, axis=spatial + 1))
    return result


def nodal_part(masked_res):
    gradient_rhs = backward_adjoint(masked_res[0], 0)
    for spatial in range(1, 3):
        gradient_rhs = gradient_rhs + backward_adjoint(masked_res[spatial], spatial)
    vector_rhs = [(masked_res[spatial] + downward(masked_res[spatial], spatial)) * 0.5 for spatial in range(3)]
    nodal_rhs = jnp.stack([gradient_rhs] + vector_rhs)
    first_node = node_damping * nodal_rhs / 7.0
    second_node = first_node + node_damping * (nodal_rhs - nodal_operator(first_node)) / 7.0
    potential = second_node[0]
    parts = [forward_diff(potential, spatial) + (second_node[spatial + 1] + upward(second_node[spatial + 1], spatial)) * 0.5 for spatial in range(3)]
    return jnp.stack(parts)


def reference(rhs, conductivity, fraction, region, flags):
    sigma = conductance(conductivity, region)[None] * fraction
    keeping = 1.0 - flags.astype(jnp.float32)
    inverse = 1.0 / (keeping * (4.0 + sigma) + (1.0 - keeping))
    first_iter = edge_damping * inverse * rhs
    second_iter = first_iter + edge_damping * inverse * (rhs - masked_operator(first_iter, keeping, sigma))
    residual = rhs - masked_operator(second_iter, keeping, sigma)
    correction = keeping * nodal_part(keeping * residual)
    return second_iter + correction
```

```python
import functools

import jax
import jax.numpy as jnp
from jax import lax
from jax.experimental import pallas as pl
from jax.experimental.pallas import tpu as pltpu
from jax.sharding import PartitionSpec as P

EDGE = 0.8
NODE = 0.8 / 7.0

BX, BY, BZ = 8, 16, 128
LOW, HIGH = 3, 4
EXT = LOW + BX + HIGH
ROWS = 6 * BY + 8
YMAIN = EXT * 24
YROWS = YMAIN + 64
VMEM_LIMIT = 16 * 1024 * 1024

VMEM = pl.BlockSpec(memory_space=pltpu.VMEM)
SMEM = pl.BlockSpec(memory_space=pltpu.SMEM)


def call(body, out_shape, n_vmem, n_smem, name, scratch=(), flops=1000000):
    return pl.pallas_call(
        body,
        out_shape=out_shape,
        in_specs=[SMEM] * n_smem + [VMEM] * n_vmem,
        out_specs=jax.tree.map(lambda _: VMEM, out_shape),
        scratch_shapes=list(scratch),
        compiler_params=pltpu.CompilerParams(vmem_limit_bytes=VMEM_LIMIT),
        cost_estimate=pl.CostEstimate(flops=flops, bytes_accessed=1000000, transcendentals=0),
        name=name,
    )


def lanes(shape):
    return lax.broadcasted_iota(jnp.int32, shape, 1)


def rotate(v, shift, axis):
    return pltpu.roll(v, shift % v.shape[axis], axis)


def prepare(cond, rhs, fraction, region, flags, sigma_out, packed_out):
    group = lanes((8, BZ)) // 8
    for x in range(BX):
        where = region[x]
        conductivity = jnp.full((BY, BZ), cond[0], jnp.float32)
        for number in range(1, 8):
            conductivity = jnp.where(where == number, cond[number], conductivity)
        packed = jnp.zeros((8, BZ), jnp.float32)
        for field in range(6):
            if field < 3:
                value = rhs[field, x]
            else:
                value = jnp.where(flags[field - 3, x] == 0, conductivity * fraction[field - 3, x], 0.0)
                sigma_out[field - 3, x] = value
            for tile in range(2):
                slot = field * 2 + tile
                moved = rotate(value[tile * 8 : tile * 8 + 8], LOW + 8 * slot, 1)
                packed = jnp.where(group == slot, moved, packed)
        packed_out[x] = packed


def send_x(zpar, rhs, sigma, first, second, up_out, down_out, packed_out):
    even = zpar[0] == 0
    below = (lanes((8, BZ)) % 8) < LOW
    for x in range(BX):
        from_high = jnp.where(even, first[1, x], second[1, x])
        from_low = jnp.where(even, second[0, x], first[0, x])
        packed = jnp.where(below, from_low, from_high)
        packed_out[x] = packed
        for out, plane in ((up_out, x - (BX - LOW)), (down_out, x)):
            if not 0 <= plane < out.shape[0]:
                continue
            for c in range(3):
                out[plane, c * BY : (c + 1) * BY] = rhs[c, x]
                out[plane, (3 + c) * BY : (4 + c) * BY] = sigma[c, x]
            out[plane, 6 * BY :] = packed


def plane_rows(p, field, rows, rhs, sigma, low, high):
    if p < LOW:
        return low[p, field * BY + rows.start : field * BY + rows.stop]
    if p >= LOW + BX:
        return high[p - LOW - BX, field * BY + rows.start : field * BY + rows.stop]
    return (rhs if field < 3 else sigma)[field % 3, p - LOW, rows]


def plane_packed(p, rows, packed, low, high):
    if p < LOW:
        return low[p, 6 * BY + rows.start : 6 * BY + rows.stop]
    if p >= LOW + BX:
        return high[p - LOW - BX, 6 * BY + rows.start : 6 * BY + rows.stop]
    return packed[p - LOW, rows]


def send_y(ypar, rhs, sigma, packed, low, high, first_out, second_out):
    def fill(top_out, bottom_out):
        for p in range(EXT):
            for out, rows, prow in ((top_out, slice(BY - 4, BY), slice(4, 8)), (bottom_out, slice(0, 4), slice(0, 4))):
                for field in range(6):
                    at = p * 24 + field * 4
                    out[at : at + 4] = plane_rows(p, field, rows, rhs, sigma, low, high)
                at = YMAIN + p * 4
                out[at : at + 4] = plane_packed(p, prow, packed, low, high)

    for out in (first_out, second_out):
        out[YMAIN + EXT * 4 :] = jnp.zeros((YROWS - YMAIN - EXT * 4, BZ), jnp.float32)

    @pl.when(ypar[0] == 0)
    def _():
        fill(first_out, second_out)

    @pl.when(ypar[0] != 0)
    def _():
        fill(second_out, first_out)


def up_y(v):
    return rotate(v, -1, 0)


def down_y(v):
    return rotate(v, 1, 0)


def up_z(v):
    return rotate(v, -1, 1)


def down_z(v):
    return rotate(v, 1, 1)


def stencil(ypar, rhs, sigma, packed, low, high, first, second, out, wide, weight, iterate, second_iter, nodal):
    even = ypar[0] == 0
    upper = lax.broadcasted_iota(jnp.int32, (8, BZ), 0) < 4

    for p in range(EXT):
        halves = []
        at = YMAIN + p * 4
        above = jnp.where(even, first[1, at : at + 4], second[1, at : at + 4])
        below = jnp.where(even, second[0, at : at + 4], first[0, at : at + 4])
        edge = jnp.concatenate([above, below], axis=0)
        edge = jnp.where(upper, edge, rotate(edge, -8, 1))
        whole = plane_packed(p, slice(0, 8), packed, low, high)
        for field in range(6):
            at = p * 24 + field * 4
            above = jnp.where(even, first[1, at : at + 4], second[1, at : at + 4])
            below = jnp.where(even, second[0, at : at + 4], first[0, at : at + 4])
            wide[field, p, 0:BY, 0:BZ] = plane_rows(p, field, slice(0, BY), rhs, sigma, low, high)
            wide[field, p, BY:24, 0:BZ] = jnp.concatenate([above, below], axis=0)
            wide[field, p, 0:8, BZ:] = rotate(whole, -(LOW + 16 * field), 1)
            wide[field, p, 8:16, BZ:] = rotate(whole, -(LOW + 16 * field + 8), 1)
            wide[field, p, 16:24, BZ:] = rotate(edge, -(LOW + 16 * field), 1)
        for c in range(3):
            s = wide[3 + c, p]
            w = jnp.where(s > 0.0, EDGE / (4.0 + s), 0.0)
            weight[c, p] = w
            iterate[c, p] = w * wide[c, p]

    def faces(u, p):
        u0, u1, u2 = u[0, p], u[1, p], u[2, p]
        f0 = (up_y(u2) - u2) - (up_z(u1) - u1)
        f1 = (up_z(u0) - u0) - (u[2, p + 1] - u2)
        f2 = (u[1, p + 1] - u1) - (up_y(u0) - u0)
        return f0, f1, f2

    def curl0(f):
        return (down_z(f[1]) - f[1]) - (down_y(f[2]) - f[2])

    def curl1(f, prev):
        return (prev[2] - f[2]) - (down_z(f[0]) - f[0])

    def curl2(f, prev):
        return (down_y(f[0]) - f[0]) - (prev[1] - f[1])

    prev = faces(iterate, 0)
    for p in range(1, EXT - 1):
        f = faces(iterate, p)
        for c, k in enumerate((curl0(f), curl1(f, prev), curl2(f, prev))):
            u = iterate[c, p]
            second_iter[c, p] = u + weight[c, p] * (wide[c, p] - (k + wide[3 + c, p] * u))
        prev = f

    def residual(c, p, k):
        s = wide[3 + c, p]
        return jnp.where(s > 0.0, wide[c, p] - (k + s * second_iter[c, p]), 0.0)

    prev = faces(second_iter, 1)
    before = residual(0, 1, curl0(prev))
    for p in range(2, EXT - 2):
        f = faces(second_iter, p)
        q0 = residual(0, p, curl0(f))
        q1 = residual(1, p, curl1(f, prev))
        q2 = residual(2, p, curl2(f, prev))
        d1, d2 = down_y(q1), down_z(q2)
        nodal[0, p] = (before - q0) + (d1 - q1) + (d2 - q2)
        nodal[1, p] = (before + q0) * 0.5
        nodal[2, p] = (d1 + q1) * 0.5
        nodal[3, p] = (d2 + q2) * 0.5
        prev, before = f, q0

    def node(c, p):
        b = nodal[c, p]
        near = (nodal[c, p - 1] + nodal[c, p + 1]) + (up_y(b) + down_y(b)) + (up_z(b) + down_z(b))
        return (1.2 * NODE) * b + (NODE * NODE) * near

    n0, n1 = node(0, LOW), node(1, LOW)
    for x in range(BX):
        p = x + LOW
        n0_next, n1_next = node(0, p + 1), node(1, p + 1)
        n2, n3 = node(2, p), node(3, p)
        corrections = (
            (n0_next - n0) + (n1_next + n1) * 0.5,
            (up_y(n0) - n0) + (n2 + up_y(n2)) * 0.5,
            (up_z(n0) - n0) + (n3 + up_z(n3)) * 0.5,
        )
        for c in range(3):
            kept = second_iter[c, p, 0:BY, 0:BZ] + corrections[c][0:BY, 0:BZ]
            out[c, x] = jnp.where(sigma[c, x] > 0.0, kept, 0.96 * rhs[c, x])
        n0, n1 = n0_next, n1_next


def pairs(count):
    return (
        [[i, i + 1] for i in range(0, count, 2)],
        [[i, (i + 1) % count] for i in range(1, count, 2)],
    )


def gather(value, axis, groups):
    return lax.all_gather(value, axis, axis=0, tiled=False, axis_index_groups=groups)


def on_device(rhs, conductivity, fraction, region, flags):
    f32 = functools.partial(jax.ShapeDtypeStruct, dtype=jnp.float32)
    parity = lambda axis: (lax.axis_index(axis) % 2).astype(jnp.int32).reshape(1)
    ypar, zpar = parity("gy"), parity("gz")

    sigma, packed = call(prepare, (f32((3, BX, BY, BZ)), f32((BX, 8, BZ))), 4, 1, "prepare")(
        conductivity, rhs, fraction, region, flags
    )
    even_z, odd_z = pairs(lax.axis_size("gz"))
    first = gather(packed, "gz", even_z)
    second = gather(packed, "gz", odd_z)

    up, down, packed = call(
        send_x, (f32((LOW, ROWS, BZ)), f32((HIGH, ROWS, BZ)), f32((BX, 8, BZ))), 4, 1, "send_x"
    )(zpar, rhs, sigma, first, second)
    count = lax.axis_size("gx")
    low = lax.ppermute(up, "gx", [(i, (i + 1) % count) for i in range(count)])
    high = lax.ppermute(down, "gx", [((i + 1) % count, i) for i in range(count)])

    even_y, odd_y = pairs(lax.axis_size("gy"))
    to_first, to_second = call(send_y, (f32((YROWS, BZ)), f32((YROWS, BZ))), 5, 1, "send_y")(
        ypar, rhs, sigma, packed, low, high
    )
    first = gather(to_first, "gy", even_y)
    second = gather(to_second, "gy", odd_y)

    wide = (EXT, 24, 2 * BZ)
    return call(
        stencil,
        f32((3, BX, BY, BZ)),
        7,
        1,
        "stencil",
        scratch=(
            pltpu.VMEM((6, *wide), jnp.float32),
            pltpu.VMEM((3, *wide), jnp.float32),
            pltpu.VMEM((3, *wide), jnp.float32),
            pltpu.VMEM((3, *wide), jnp.float32),
            pltpu.VMEM((4, *wide), jnp.float32),
        ),
    )(ypar, rhs, sigma, packed, low, high, first, second)


def solution(mesh):
    return jax.shard_map(
        on_device,
        mesh=mesh,
        in_specs=(
            P(None, "gx", "gy", "gz"),
            P(),
            P(None, "gx", "gy", "gz"),
            P("gx", "gy", "gz"),
            P(None, "gx", "gy", "gz"),
        ),
        out_specs=P(None, "gx", "gy", "gz"),
        check_vma=False,
    )
```

```python
import functools

import jax
import jax.numpy as jnp
import numpy as np
from jax import lax
from jax.experimental import pallas as pl
from jax.experimental.pallas import tpu as pltpu
from jax.sharding import PartitionSpec as P

EDGE = 0.8
NODE = 0.8 / 7.0

BX, BY, BZ = 8, 16, 128
LOW, HIGH = 3, 4
EXT = LOW + BX + HIGH
VMEM_LIMIT = 16 * 1024 * 1024

VMEM = pl.BlockSpec(memory_space=pltpu.VMEM)
SMEM = pl.BlockSpec(memory_space=pltpu.SMEM)
HBM = pl.BlockSpec(memory_space=pltpu.HBM)


def halo_need():
    size = BX + 9

    def at(need, axis, k):
        return np.roll(need, k, axis)

    out = np.zeros((3, size, size, size), bool)
    out[:, 4 : 4 + BX, 4 : 4 + BX, 4 : 4 + BX] = True
    node = np.zeros((4, size, size, size), bool)
    for a in range(3):
        both = out[a] | at(out[a], a, 1)
        node[0] |= both
        node[a + 1] |= both
    near = node.copy()
    for a in range(3):
        near |= np.roll(node, 1, a + 1) | np.roll(node, -1, a + 1)
    masked = np.stack([near[0] | at(near[0], a, -1) | near[a + 1] | at(near[a + 1], a, -1) for a in range(3)])

    def operand(need):
        face = np.zeros_like(need)
        for a in range(3):
            b, c = (a + 1) % 3, (a + 2) % 3
            face[b] |= need[a] | at(need[a], c, -1)
            face[c] |= need[a] | at(need[a], b, -1)
        edge = need.copy()
        for a in range(3):
            b, c = (a + 1) % 3, (a + 2) % 3
            edge[b] |= face[a] | at(face[a], c, 1)
            edge[c] |= face[a] | at(face[a], b, 1)
        return edge

    second = operand(masked) | out
    first = operand(second)
    return second.any(3).astype(int) + first.any(3).astype(int)


NEED = halo_need()


def plane_need(c, p):
    return NEED[c, p - LOW + 4].max()


def row_counts(c, p):
    need = NEED[c, p - LOW + 4]
    below, above = need[:4], need[4 + BX :]
    return tuple((int((side > 0).sum()), int((side > 1).sum())) for side in (below, above))


def x_layout(planes):
    at, rows = {}, 0
    for p in planes:
        for field in range(6):
            if plane_need(field % 3, p) > field // 3:
                at[p, field] = rows
                rows += BY
    for p in planes:
        at[p, "packed"] = rows
        rows += 8
    return at, rows


X_LOW, X_LOW_ROWS = x_layout(range(LOW))
X_HIGH, X_HIGH_ROWS = x_layout(range(LOW + BX, EXT))


def y_layout(side):
    at, rows = {}, 0
    for p in range(EXT):
        for field in range(6):
            count = row_counts(field % 3, p)[side][field // 3]
            at[p, field] = (rows, count)
            rows += count
    rows = -(-rows // 8) * 8
    for p in range(0, EXT, 2):
        at[p, "packed"] = at[p + 1, "packed"] = rows
        rows += 4
    return at, rows


Y_LOW, Y_LOW_ROWS = y_layout(0)
Y_HIGH, Y_HIGH_ROWS = y_layout(1)
Y_ROWS = -(-max(Y_LOW_ROWS, Y_HIGH_ROWS) // 8) * 8


def call(body, out_shape, specs, name, scratch=(), flops=1000000):
    return pl.pallas_call(
        body,
        out_shape=out_shape,
        in_specs=specs,
        out_specs=jax.tree.map(lambda _: VMEM, out_shape),
        scratch_shapes=list(scratch),
        compiler_params=pltpu.CompilerParams(vmem_limit_bytes=VMEM_LIMIT),
        cost_estimate=pl.CostEstimate(flops=flops, bytes_accessed=1000000, transcendentals=0),
        name=name,
    )


def lanes(shape):
    return lax.broadcasted_iota(jnp.int32, shape, 1)


def rotate(v, shift, axis):
    return pltpu.roll(v, shift % v.shape[axis], axis)


def weigh(sigma):
    return jnp.where(sigma > 0.0, EDGE / (4.0 + sigma), 0.0)


def prepare(cond_in, rhs_in, fraction_in, region_in, flags_in, rhs, sigma, first_iter, packed_out, cond, fraction, region, flags, sems):
    copies = [
        pltpu.make_async_copy(source, target, sems.at[i])
        for i, (source, target) in enumerate(
            ((cond_in, cond), (region_in, region), (fraction_in, fraction), (flags_in, flags), (rhs_in, rhs))
        )
    ]
    for copy in copies:
        copy.start()
    for copy in copies:
        copy.wait()
    group = lanes((8, BZ)) // 8
    for x in range(BX):
        where = region[x]
        conductivity = jnp.full((BY, BZ), cond[0], jnp.float32)
        for number in range(1, 8):
            conductivity = jnp.where(where == number, cond[number], conductivity)
        packed = jnp.zeros((8, BZ), jnp.float32)
        for field in range(6):
            if field < 3:
                value = rhs[field, x]
            else:
                c = field - 3
                value = jnp.where(flags[c, x] == 0, conductivity * fraction[c, x], 0.0)
                sigma[c, x] = value
                first_iter[c, x] = weigh(value) * rhs[c, x]
            for tile in range(2):
                slot = field * 2 + tile
                moved = rotate(value[tile * 8 : tile * 8 + 8], LOW + 8 * slot, 1)
                packed = jnp.where(group == slot, moved, packed)
        packed_out[x] = packed


def send_x(zpar, rhs, sigma, first_iter, first, second, up_out, down_out, packed_out):
    even = zpar[0] == 0
    below = (lanes((8, BZ)) % 8) < LOW
    for x in range(BX):
        from_high = jnp.where(even, first[1, x], second[1, x])
        from_low = jnp.where(even, second[0, x], first[0, x])
        packed_out[x] = jnp.where(below, from_low, from_high)
    for out, layout, shift in ((up_out, X_LOW, BX), (down_out, X_HIGH, -BX)):
        for (p, field), at in layout.items():
            x = p - LOW + shift
            if field == "packed":
                out[at : at + 8] = packed_out[x]
            elif field >= 3:
                out[at : at + BY] = sigma[field - 3, x]
            else:
                out[at : at + BY] = (rhs if plane_need(field, p) == 2 else first_iter)[field, x]


def plane_rows(p, field, start, stop, rhs, sigma, low, high):
    if p < LOW:
        at = X_LOW[p, field]
        return low[at + start : at + stop]
    if p >= LOW + BX:
        at = X_HIGH[p, field]
        return high[at + start : at + stop]
    return (rhs if field < 3 else sigma)[field % 3, p - LOW, start:stop]


def plane_packed(p, start, stop, packed, low, high):
    if p < LOW:
        at = X_LOW[p, "packed"]
        return low[at + start : at + stop]
    if p >= LOW + BX:
        at = X_HIGH[p, "packed"]
        return high[at + start : at + stop]
    return packed[p - LOW, start:stop]


def send_y(ypar, rhs, sigma, first_iter, packed, low, high, first_out, second_out):
    swap = (lanes((4, BZ)) // 8) % 2

    def first_rows(p, c, start, stop):
        if LOW <= p < LOW + BX:
            return first_iter[c, p - LOW, start:stop]
        value = plane_rows(p, c, start, stop, rhs, sigma, low, high)
        if plane_need(c, p) == 2:
            value = weigh(plane_rows(p, c + 3, start, stop, rhs, sigma, low, high)) * value
        return value

    def fill(out, layout, side):
        for p in range(EXT):
            for field in range(6):
                at, count = layout[p, field]
                both = layout[p, field % 3 + 3][1]
                if field >= 3 and count:
                    start = 0 if side else BY - count
                    out[at : at + count] = plane_rows(p, field, start, start + count, rhs, sigma, low, high)
                if field < 3 and both:
                    start = 0 if side else BY - both
                    place = at if side else at + count - both
                    out[place : place + both] = plane_rows(p, field, start, start + both, rhs, sigma, low, high)
                if field < 3 and count > both:
                    start = both if side else BY - count
                    place = at + both if side else at
                    out[place : place + count - both] = first_rows(p, field, start, start + count - both)
        start = 0 if side else 4
        for p in range(0, EXT, 2):
            value = plane_packed(p, start, start + 4, packed, low, high)
            if p + 1 < EXT:
                other = plane_packed(p + 1, start, start + 4, packed, low, high)
                value = jnp.where(swap == 1 - side, value, rotate(other, 8 if side else -8, 1))
            at = layout[p, "packed"]
            out[at : at + 4] = value

    @pl.when(ypar[0] == 0)
    def _():
        fill(first_out, Y_LOW, 0)
        fill(second_out, Y_HIGH, 1)

    @pl.when(ypar[0] != 0)
    def _():
        fill(second_out, Y_LOW, 0)
        fill(first_out, Y_HIGH, 1)


def up_y(v):
    return rotate(v, -1, 0)


def down_y(v):
    return rotate(v, 1, 0)


def up_z(v):
    return rotate(v, -1, 1)


def down_z(v):
    return rotate(v, 1, 1)


def stencil(ypar, rhs, sigma, first_iter, packed, low, high, first, second, out, wide, weight, iterate, second_iter, nodal):
    even = ypar[0] == 0
    row8 = lax.broadcasted_iota(jnp.int32, (8, BZ), 0)

    for p in range(EXT):
        at_low, at_high = Y_LOW[p, "packed"], Y_HIGH[p, "packed"]
        edge = jnp.concatenate(
            [
                jnp.where(even, first[1, at_high : at_high + 4], second[1, at_high : at_high + 4]),
                jnp.where(even, second[0, at_low : at_low + 4], first[0, at_low : at_low + 4]),
            ],
            axis=0,
        )
        edge = jnp.where((row8 < 4) == (p % 2 == 0), edge, rotate(edge, -8, 1))
        whole = plane_packed(p, 0, 8, packed, low, high)
        for field in range(6):
            c = field % 3
            if plane_need(c, p) == 0:
                continue
            if plane_need(c, p) > field // 3:
                wide[field, p, 0:BY, 0:BZ] = plane_rows(p, field, 0, BY, rhs, sigma, low, high)
                at, count = Y_HIGH[p, field]
                if count:
                    wide[field, p, BY : BY + count, 0:BZ] = jnp.where(
                        even, first[1, at : at + count], second[1, at : at + count]
                    )
                at, count = Y_LOW[p, field]
                if count:
                    wide[field, p, 24 - count : 24, 0:BZ] = jnp.where(
                        even, second[0, at : at + count], first[0, at : at + count]
                    )
            wide[field, p, 0:8, BZ:] = rotate(whole, -(LOW + 16 * field), 1)
            wide[field, p, 8:16, BZ:] = rotate(whole, -(LOW + 16 * field + 8), 1)
            wide[field, p, 16:24, BZ:] = rotate(edge, -(LOW + 16 * field), 1)
        for c in range(3):
            if plane_need(c, p) == 0:
                continue
            if plane_need(c, p) == 1:
                iterate[c, p, :, 0:BZ] = wide[c, p, :, 0:BZ]
                iterate[c, p, :, BZ:] = weigh(wide[3 + c, p, :, BZ:]) * wide[c, p, :, BZ:]
                continue
            w = weigh(wide[3 + c, p])
            weight[c, p] = w
            iterate[c, p] = w * wide[c, p]
            (low_any, low_both), (high_any, high_both) = row_counts(c, p)
            for start, stop in ((BY + high_both, BY + high_any), (24 - low_any, 24 - low_both)):
                if start < stop:
                    iterate[c, p, start:stop, 0:BZ] = wide[c, p, start:stop, 0:BZ]

    def faces(u, p):
        u0, u1, u2 = u[0, p], u[1, p], u[2, p]
        f0 = (up_y(u2) - u2) - (up_z(u1) - u1)
        f1 = (up_z(u0) - u0) - (u[2, p + 1] - u2)
        f2 = (u[1, p + 1] - u1) - (up_y(u0) - u0)
        return f0, f1, f2

    def curl0(f):
        return (down_z(f[1]) - f[1]) - (down_y(f[2]) - f[2])

    def curl1(f, prev):
        return (prev[2] - f[2]) - (down_z(f[0]) - f[0])

    def curl2(f, prev):
        return (down_y(f[0]) - f[0]) - (prev[1] - f[1])

    prev = faces(iterate, 0)
    for p in range(1, EXT - 1):
        f = faces(iterate, p)
        for c, k in enumerate((curl0(f), curl1(f, prev), curl2(f, prev))):
            u = iterate[c, p]
            second_iter[c, p] = u + weight[c, p] * (wide[c, p] - (k + wide[3 + c, p] * u))
        prev = f

    def residual(c, p, k):
        s = wide[3 + c, p]
        return jnp.where(s > 0.0, wide[c, p] - (k + s * second_iter[c, p]), 0.0)

    prev = faces(second_iter, 1)
    before = residual(0, 1, curl0(prev))
    for p in range(2, EXT - 2):
        f = faces(second_iter, p)
        q0 = residual(0, p, curl0(f))
        q1 = residual(1, p, curl1(f, prev))
        q2 = residual(2, p, curl2(f, prev))
        d1, d2 = down_y(q1), down_z(q2)
        nodal[0, p] = (before - q0) + (d1 - q1) + (d2 - q2)
        nodal[1, p] = (before + q0) * 0.5
        nodal[2, p] = (d1 + q1) * 0.5
        nodal[3, p] = (d2 + q2) * 0.5
        prev, before = f, q0

    def node(c, p):
        b = nodal[c, p]
        near = (nodal[c, p - 1] + nodal[c, p + 1]) + (up_y(b) + down_y(b)) + (up_z(b) + down_z(b))
        return (1.2 * NODE) * b + (NODE * NODE) * near

    n0, n1 = node(0, LOW), node(1, LOW)
    for x in range(BX):
        p = x + LOW
        n0_next, n1_next = node(0, p + 1), node(1, p + 1)
        n2, n3 = node(2, p), node(3, p)
        corrections = (
            (n0_next - n0) + (n1_next + n1) * 0.5,
            (up_y(n0) - n0) + (n2 + up_y(n2)) * 0.5,
            (up_z(n0) - n0) + (n3 + up_z(n3)) * 0.5,
        )
        for c in range(3):
            kept = second_iter[c, p, 0:BY, 0:BZ] + corrections[c][0:BY, 0:BZ]
            out[c, x] = jnp.where(sigma[c, x] > 0.0, kept, 0.96 * rhs[c, x])
        n0, n1 = n0_next, n1_next


def pairs(count):
    return (
        [[i, i + 1] for i in range(0, count, 2)],
        [[i, (i + 1) % count] for i in range(1, count, 2)],
    )


def gather(value, axis, groups):
    return lax.all_gather(value, axis, axis=0, tiled=False, axis_index_groups=groups)


def on_device(rhs, conductivity, fraction, region, flags):
    f32 = functools.partial(jax.ShapeDtypeStruct, dtype=jnp.float32)
    parity = lambda axis: (lax.axis_index(axis) % 2).astype(jnp.int32).reshape(1)
    ypar, zpar = parity("gy"), parity("gz")

    block = f32((3, BX, BY, BZ))
    rhs, sigma, first_iter, packed = call(
        prepare,
        (block, block, block, f32((BX, 8, BZ))),
        [HBM] * 5,
        "prepare",
        scratch=(
            pltpu.SMEM((8,), jnp.float32),
            pltpu.VMEM((3, BX, BY, BZ), jnp.float32),
            pltpu.VMEM((BX, BY, BZ), jnp.int32),
            pltpu.VMEM((3, BX, BY, BZ), jnp.int32),
            pltpu.SemaphoreType.DMA((5,)),
        ),
    )(conductivity, rhs, fraction, region, flags)
    even_z, odd_z = pairs(lax.axis_size("gz"))
    first = gather(packed, "gz", even_z)
    second = gather(packed, "gz", odd_z)

    up, down, packed = call(
        send_x, (f32((X_LOW_ROWS, BZ)), f32((X_HIGH_ROWS, BZ)), f32((BX, 8, BZ))), [SMEM] + [VMEM] * 5, "send_x"
    )(zpar, rhs, sigma, first_iter, first, second)
    count = lax.axis_size("gx")
    low = lax.ppermute(up, "gx", [(i, (i + 1) % count) for i in range(count)])
    high = lax.ppermute(down, "gx", [((i + 1) % count, i) for i in range(count)])

    even_y, odd_y = pairs(lax.axis_size("gy"))
    to_first, to_second = call(
        send_y, (f32((Y_ROWS, BZ)), f32((Y_ROWS, BZ))), [SMEM] + [VMEM] * 6, "send_y"
    )(ypar, rhs, sigma, first_iter, packed, low, high)
    first = gather(to_first, "gy", even_y)
    second = gather(to_second, "gy", odd_y)

    wide = (EXT, 24, 2 * BZ)
    return call(
        stencil,
        block,
        [SMEM] + [VMEM] * 8,
        "stencil",
        scratch=(
            pltpu.VMEM((6, *wide), jnp.float32),
            pltpu.VMEM((3, *wide), jnp.float32),
            pltpu.VMEM((3, *wide), jnp.float32),
            pltpu.VMEM((3, *wide), jnp.float32),
            pltpu.VMEM((4, *wide), jnp.float32),
        ),
    )(ypar, rhs, sigma, first_iter, packed, low, high, first, second)


def solution(mesh):
    return jax.shard_map(
        on_device,
        mesh=mesh,
        in_specs=(
            P(None, "gx", "gy", "gz"),
            P(),
            P(None, "gx", "gy", "gz"),
            P("gx", "gy", "gz"),
            P(None, "gx", "gy", "gz"),
        ),
        out_specs=P(None, "gx", "gy", "gz"),
        check_vma=False,
    )
```

```python
import functools

import jax
import jax.numpy as jnp
import numpy as np
from jax import lax
from jax.experimental import pallas as pl
from jax.experimental.pallas import tpu as pltpu
from jax.sharding import PartitionSpec as P

EDGE = 0.8
NODE = 0.8 / 7.0

BX, BY, BZ = 8, 16, 128
LOW, HIGH = 3, 4
EXT = LOW + BX + HIGH
VMEM_LIMIT = 16 * 1024 * 1024

VMEM = pl.BlockSpec(memory_space=pltpu.VMEM)
SMEM = pl.BlockSpec(memory_space=pltpu.SMEM)
HBM = pl.BlockSpec(memory_space=pltpu.HBM)


def halo_need():
    size = BX + 9

    def at(need, axis, k):
        return np.roll(need, k, axis)

    out = np.zeros((3, size, size, size), bool)
    out[:, 4 : 4 + BX, 4 : 4 + BX, 4 : 4 + BX] = True
    node = np.zeros((4, size, size, size), bool)
    for a in range(3):
        both = out[a] | at(out[a], a, 1)
        node[0] |= both
        node[a + 1] |= both
    near = node.copy()
    for a in range(3):
        near |= np.roll(node, 1, a + 1) | np.roll(node, -1, a + 1)
    masked = np.stack([near[0] | at(near[0], a, -1) | near[a + 1] | at(near[a + 1], a, -1) for a in range(3)])

    def operand(need):
        face = np.zeros_like(need)
        for a in range(3):
            b, c = (a + 1) % 3, (a + 2) % 3
            face[b] |= need[a] | at(need[a], c, -1)
            face[c] |= need[a] | at(need[a], b, -1)
        edge = need.copy()
        for a in range(3):
            b, c = (a + 1) % 3, (a + 2) % 3
            edge[b] |= face[a] | at(face[a], c, 1)
            edge[c] |= face[a] | at(face[a], b, 1)
        return edge

    second = operand(masked) | out
    first = operand(second)
    return second.any(3).astype(int) + first.any(3).astype(int)


NEED = halo_need()


def plane_need(c, p):
    return NEED[c, p - LOW + 4].max()


def row_counts(c, p):
    need = NEED[c, p - LOW + 4]
    below, above = need[:4], need[4 + BX :]
    return tuple((int((side > 0).sum()), int((side > 1).sum())) for side in (below, above))


def x_layout(planes):
    at, rows = {}, 0
    for p in planes:
        for field in range(6):
            if plane_need(field % 3, p) > field // 3:
                at[p, field] = rows
                rows += BY
    for p in planes:
        at[p, "packed"] = rows
        rows += 8
    return at, rows


X_LOW, X_LOW_ROWS = x_layout(range(LOW))
X_HIGH, X_HIGH_ROWS = x_layout(range(LOW + BX, EXT))


def y_layout(side):
    at, rows = {}, 0
    for p in range(EXT):
        for field in range(6):
            count = row_counts(field % 3, p)[side][field // 3]
            at[p, field] = (rows, count)
            rows += count
    rows = -(-rows // 8) * 8
    for p in range(0, EXT, 2):
        at[p, "packed"] = at[p + 1, "packed"] = rows
        rows += 4
    return at, rows


Y_LOW, Y_LOW_ROWS = y_layout(0)
Y_HIGH, Y_HIGH_ROWS = y_layout(1)
Y_ROWS = -(-max(Y_LOW_ROWS, Y_HIGH_ROWS) // 8) * 8


def call(body, out_shape, specs, name, scratch=(), flops=1000000):
    return pl.pallas_call(
        body,
        out_shape=out_shape,
        in_specs=specs,
        out_specs=jax.tree.map(lambda _: VMEM, out_shape),
        scratch_shapes=list(scratch),
        compiler_params=pltpu.CompilerParams(vmem_limit_bytes=VMEM_LIMIT),
        cost_estimate=pl.CostEstimate(flops=flops, bytes_accessed=1000000, transcendentals=0),
        name=name,
    )


def lanes(shape):
    return lax.broadcasted_iota(jnp.int32, shape, 1)


def rotate(v, shift, axis):
    return pltpu.roll(v, shift % v.shape[axis], axis)


def weigh(sigma):
    return jnp.where(sigma > 0.0, EDGE / (4.0 + sigma), 0.0)


def prepare(cond_in, rhs_in, fraction_in, region_in, flags_in, rhs, sigma, first_iter, packed_out, cond, fraction, region, flags, sems):
    copies = [
        pltpu.make_async_copy(source, target, sems.at[i])
        for i, (source, target) in enumerate(
            ((cond_in, cond), (region_in, region), (fraction_in, fraction), (flags_in, flags), (rhs_in, rhs))
        )
    ]
    for copy in copies:
        copy.start()
    for copy in copies:
        copy.wait()
    group = lanes((8, BZ)) // 8
    for x in range(BX):
        where = region[x]
        conductivity = jnp.full((BY, BZ), cond[0], jnp.float32)
        for number in range(1, 8):
            conductivity = jnp.where(where == number, cond[number], conductivity)
        packed = jnp.zeros((8, BZ), jnp.float32)
        for field in range(6):
            if field < 3:
                value = rhs[field, x]
            else:
                c = field - 3
                value = jnp.where(flags[c, x] == 0, conductivity * fraction[c, x], 0.0)
                sigma[c, x] = value
                first_iter[c, x] = weigh(value) * rhs[c, x]
            for tile in range(2):
                slot = field * 2 + tile
                moved = rotate(value[tile * 8 : tile * 8 + 8], LOW + 8 * slot, 1)
                packed = jnp.where(group == slot, moved, packed)
        packed_out[x] = packed


def send_x(zpar, rhs, sigma, first_iter, first, second, up_out, down_out, packed_out):
    even = zpar[0] == 0
    below = (lanes((8, BZ)) % 8) < LOW
    for x in range(BX):
        from_high = jnp.where(even, first[1, x], second[1, x])
        from_low = jnp.where(even, second[0, x], first[0, x])
        packed_out[x] = jnp.where(below, from_low, from_high)
    for out, layout, shift in ((up_out, X_LOW, BX), (down_out, X_HIGH, -BX)):
        for (p, field), at in layout.items():
            x = p - LOW + shift
            if field == "packed":
                out[at : at + 8] = packed_out[x]
            elif field >= 3:
                out[at : at + BY] = sigma[field - 3, x]
            else:
                out[at : at + BY] = (rhs if plane_need(field, p) == 2 else first_iter)[field, x]


def plane_rows(p, field, start, stop, rhs, sigma, low, high):
    if p < LOW:
        at = X_LOW[p, field]
        return low[at + start : at + stop]
    if p >= LOW + BX:
        at = X_HIGH[p, field]
        return high[at + start : at + stop]
    return (rhs if field < 3 else sigma)[field % 3, p - LOW, start:stop]


def plane_packed(p, start, stop, packed, low, high):
    if p < LOW:
        at = X_LOW[p, "packed"]
        return low[at + start : at + stop]
    if p >= LOW + BX:
        at = X_HIGH[p, "packed"]
        return high[at + start : at + stop]
    return packed[p - LOW, start:stop]


def send_y(ypar, rhs, sigma, first_iter, packed, low, high, first_out, second_out):
    swap = (lanes((4, BZ)) // 8) % 2

    def first_rows(p, c, start, stop):
        if LOW <= p < LOW + BX:
            return first_iter[c, p - LOW, start:stop]
        value = plane_rows(p, c, start, stop, rhs, sigma, low, high)
        if plane_need(c, p) == 2:
            value = weigh(plane_rows(p, c + 3, start, stop, rhs, sigma, low, high)) * value
        return value

    def fill(out, layout, side):
        for p in range(EXT):
            for field in range(6):
                at, count = layout[p, field]
                both = layout[p, field % 3 + 3][1]
                if field >= 3 and count:
                    start = 0 if side else BY - count
                    out[at : at + count] = plane_rows(p, field, start, start + count, rhs, sigma, low, high)
                if field < 3 and both:
                    start = 0 if side else BY - both
                    place = at if side else at + count - both
                    out[place : place + both] = plane_rows(p, field, start, start + both, rhs, sigma, low, high)
                if field < 3 and count > both:
                    start = both if side else BY - count
                    place = at + both if side else at
                    out[place : place + count - both] = first_rows(p, field, start, start + count - both)
        start = 0 if side else 4
        for p in range(0, EXT, 2):
            value = plane_packed(p, start, start + 4, packed, low, high)
            if p + 1 < EXT:
                other = plane_packed(p + 1, start, start + 4, packed, low, high)
                value = jnp.where(swap == 1 - side, value, rotate(other, 8 if side else -8, 1))
            at = layout[p, "packed"]
            out[at : at + 4] = value

    @pl.when(ypar[0] == 0)
    def _():
        fill(first_out, Y_LOW, 0)
        fill(second_out, Y_HIGH, 1)

    @pl.when(ypar[0] != 0)
    def _():
        fill(second_out, Y_LOW, 0)
        fill(first_out, Y_HIGH, 1)


def up_y(v):
    return rotate(v, -1, 0)


def down_y(v):
    return rotate(v, 1, 0)


def up_z(v):
    return rotate(v, -1, 1)


def down_z(v):
    return rotate(v, 1, 1)


def stencil(ypar, rhs, sigma, first_iter, packed, low, high, first, second, out, wide, weight, iterate, second_iter, nodal):
    even = ypar[0] == 0
    row8 = lax.broadcasted_iota(jnp.int32, (8, BZ), 0)

    for p in range(EXT):
        at_low, at_high = Y_LOW[p, "packed"], Y_HIGH[p, "packed"]
        edge = jnp.concatenate(
            [
                jnp.where(even, first[1, at_high : at_high + 4], second[1, at_high : at_high + 4]),
                jnp.where(even, second[0, at_low : at_low + 4], first[0, at_low : at_low + 4]),
            ],
            axis=0,
        )
        edge = jnp.where((row8 < 4) == (p % 2 == 0), edge, rotate(edge, -8, 1))
        whole = plane_packed(p, 0, 8, packed, low, high)
        for field in range(6):
            c = field % 3
            if plane_need(c, p) == 0:
                continue
            if plane_need(c, p) > field // 3:
                wide[field, p, 0:BY, 0:BZ] = plane_rows(p, field, 0, BY, rhs, sigma, low, high)
                at, count = Y_HIGH[p, field]
                if count:
                    wide[field, p, BY : BY + count, 0:BZ] = jnp.where(
                        even, first[1, at : at + count], second[1, at : at + count]
                    )
                at, count = Y_LOW[p, field]
                if count:
                    wide[field, p, 24 - count : 24, 0:BZ] = jnp.where(
                        even, second[0, at : at + count], first[0, at : at + count]
                    )
            wide[field, p, 0:8, BZ:] = rotate(whole, -(LOW + 16 * field), 1)
            wide[field, p, 8:16, BZ:] = rotate(whole, -(LOW + 16 * field + 8), 1)
            wide[field, p, 16:24, BZ:] = rotate(edge, -(LOW + 16 * field), 1)
        for c in range(3):
            if plane_need(c, p) == 0:
                continue
            if plane_need(c, p) == 1:
                iterate[c, p, :, 0:BZ] = wide[c, p, :, 0:BZ]
                iterate[c, p, :, BZ:] = weigh(wide[3 + c, p, :, BZ:]) * wide[c, p, :, BZ:]
                continue
            w = weigh(wide[3 + c, p])
            weight[c, p] = w
            iterate[c, p] = w * wide[c, p]
            (low_any, low_both), (high_any, high_both) = row_counts(c, p)
            for start, stop in ((BY + high_both, BY + high_any), (24 - low_any, 24 - low_both)):
                if start < stop:
                    iterate[c, p, start:stop, 0:BZ] = wide[c, p, start:stop, 0:BZ]

    def faces(u, p):
        u0, u1, u2 = u[0, p], u[1, p], u[2, p]
        f0 = (up_y(u2) - u2) - (up_z(u1) - u1)
        f1 = (up_z(u0) - u0) - (u[2, p + 1] - u2)
        f2 = (u[1, p + 1] - u1) - (up_y(u0) - u0)
        return f0, f1, f2

    def curl0(f):
        return (down_z(f[1]) - f[1]) - (down_y(f[2]) - f[2])

    def curl1(f, prev):
        return (prev[2] - f[2]) - (down_z(f[0]) - f[0])

    def curl2(f, prev):
        return (down_y(f[0]) - f[0]) - (prev[1] - f[1])

    prev = faces(iterate, 0)
    for p in range(1, EXT - 1):
        f = faces(iterate, p)
        for c, k in enumerate((curl0(f), curl1(f, prev), curl2(f, prev))):
            u = iterate[c, p]
            second_iter[c, p] = u + weight[c, p] * (wide[c, p] - (k + wide[3 + c, p] * u))
        prev = f

    def residual(c, p, k):
        s = wide[3 + c, p]
        return jnp.where(s > 0.0, wide[c, p] - (k + s * second_iter[c, p]), 0.0)

    prev = faces(second_iter, 1)
    before = residual(0, 1, curl0(prev))
    for p in range(2, EXT - 2):
        f = faces(second_iter, p)
        q0 = residual(0, p, curl0(f))
        q1 = residual(1, p, curl1(f, prev))
        q2 = residual(2, p, curl2(f, prev))
        d1, d2 = down_y(q1), down_z(q2)
        nodal[0, p] = (before - q0) + (d1 - q1) + (d2 - q2)
        nodal[1, p] = (before + q0) * 0.5
        nodal[2, p] = (d1 + q1) * 0.5
        nodal[3, p] = (d2 + q2) * 0.5
        prev, before = f, q0

    def node(c, p):
        b = nodal[c, p]
        near = (nodal[c, p - 1] + nodal[c, p + 1]) + (up_y(b) + down_y(b)) + (up_z(b) + down_z(b))
        return (1.2 * NODE) * b + (NODE * NODE) * near

    n0, n1 = node(0, LOW), node(1, LOW)
    for x in range(BX):
        p = x + LOW
        n0_next, n1_next = node(0, p + 1), node(1, p + 1)
        n2, n3 = node(2, p), node(3, p)
        corrections = (
            (n0_next - n0) + (n1_next + n1) * 0.5,
            (up_y(n0) - n0) + (n2 + up_y(n2)) * 0.5,
            (up_z(n0) - n0) + (n3 + up_z(n3)) * 0.5,
        )
        for c in range(3):
            kept = second_iter[c, p, 0:BY, 0:BZ] + corrections[c][0:BY, 0:BZ]
            out[c, x] = jnp.where(sigma[c, x] > 0.0, kept, 0.96 * rhs[c, x])
        n0, n1 = n0_next, n1_next


def pairs(count):
    return (
        [[i, i + 1] for i in range(0, count, 2)],
        [[i, (i + 1) % count] for i in range(1, count, 2)],
    )


def gather(value, axis, groups):
    return lax.all_gather(value, axis, axis=0, tiled=False, axis_index_groups=groups)


def on_device(rhs, conductivity, fraction, region, flags):
    f32 = functools.partial(jax.ShapeDtypeStruct, dtype=jnp.float32)
    parity = lambda axis: (lax.axis_index(axis) % 2).astype(jnp.int32).reshape(1)
    ypar, zpar = parity("gy"), parity("gz")

    block = f32((3, BX, BY, BZ))
    rhs, sigma, first_iter, packed = call(
        prepare,
        (block, block, block, f32((BX, 8, BZ))),
        [HBM] * 5,
        "prepare",
        scratch=(
            pltpu.SMEM((8,), jnp.float32),
            pltpu.VMEM((3, BX, BY, BZ), jnp.float32),
            pltpu.VMEM((BX, BY, BZ), jnp.int32),
            pltpu.VMEM((3, BX, BY, BZ), jnp.int32),
            pltpu.SemaphoreType.DMA((5,)),
        ),
    )(*(pltpu.with_memory_space_constraint(a, pltpu.HBM) for a in (conductivity, rhs, fraction, region, flags)))
    even_z, odd_z = pairs(lax.axis_size("gz"))
    first = gather(packed, "gz", even_z)
    second = gather(packed, "gz", odd_z)

    up, down, packed = call(
        send_x, (f32((X_LOW_ROWS, BZ)), f32((X_HIGH_ROWS, BZ)), f32((BX, 8, BZ))), [SMEM] + [VMEM] * 5, "send_x"
    )(zpar, rhs, sigma, first_iter, first, second)
    count = lax.axis_size("gx")
    low = lax.ppermute(up, "gx", [(i, (i + 1) % count) for i in range(count)])
    high = lax.ppermute(down, "gx", [((i + 1) % count, i) for i in range(count)])

    even_y, odd_y = pairs(lax.axis_size("gy"))
    to_first, to_second = call(
        send_y, (f32((Y_ROWS, BZ)), f32((Y_ROWS, BZ))), [SMEM] + [VMEM] * 6, "send_y"
    )(ypar, rhs, sigma, first_iter, packed, low, high)
    first = gather(to_first, "gy", even_y)
    second = gather(to_second, "gy", odd_y)

    wide = (EXT, 24, 2 * BZ)
    return call(
        stencil,
        block,
        [SMEM] + [VMEM] * 8,
        "stencil",
        scratch=(
            pltpu.VMEM((6, *wide), jnp.float32),
            pltpu.VMEM((3, *wide), jnp.float32),
            pltpu.VMEM((3, *wide), jnp.float32),
            pltpu.VMEM((3, *wide), jnp.float32),
            pltpu.VMEM((4, *wide), jnp.float32),
        ),
    )(ypar, rhs, sigma, first_iter, packed, low, high, first, second)


def solution(mesh):
    return jax.shard_map(
        on_device,
        mesh=mesh,
        in_specs=(
            P(None, "gx", "gy", "gz"),
            P(),
            P(None, "gx", "gy", "gz"),
            P("gx", "gy", "gz"),
            P(None, "gx", "gy", "gz"),
        ),
        out_specs=P(None, "gx", "gy", "gz"),
        check_vma=False,
    )
```

```python
import functools

import jax
import jax.numpy as jnp
import numpy as np
from jax import lax
from jax.experimental import pallas as pl
from jax.experimental.pallas import tpu as pltpu
from jax.sharding import PartitionSpec as P


EDGE = 0.8
NODE = 0.8 / 7.0

BX, BY, BZ = 8, 16, 128
LOW, HIGH = 3, 4
EXT = LOW + BX + HIGH
VMEM_LIMIT = 16 * 1024 * 1024

VMEM = pl.BlockSpec(memory_space=pltpu.VMEM)
SMEM = pl.BlockSpec(memory_space=pltpu.SMEM)
HBM = pl.BlockSpec(memory_space=pltpu.HBM)


def halo_need():
    size = BX + 9

    def at(need, axis, k):
        return np.roll(need, k, axis)

    out = np.zeros((3, size, size, size), bool)
    out[:, 4 : 4 + BX, 4 : 4 + BX, 4 : 4 + BX] = True
    node = np.zeros((4, size, size, size), bool)
    for a in range(3):
        both = out[a] | at(out[a], a, 1)
        node[0] |= both
        node[a + 1] |= both
    near = node.copy()
    for a in range(3):
        near |= np.roll(node, 1, a + 1) | np.roll(node, -1, a + 1)
    masked = np.stack([near[0] | at(near[0], a, -1) | near[a + 1] | at(near[a + 1], a, -1) for a in range(3)])

    def operand(need):
        face = np.zeros_like(need)
        for a in range(3):
            b, c = (a + 1) % 3, (a + 2) % 3
            face[b] |= need[a] | at(need[a], c, -1)
            face[c] |= need[a] | at(need[a], b, -1)
        edge = need.copy()
        for a in range(3):
            b, c = (a + 1) % 3, (a + 2) % 3
            edge[b] |= face[a] | at(face[a], c, 1)
            edge[c] |= face[a] | at(face[a], b, 1)
        return edge

    second = operand(masked) | out
    first = operand(second)
    return second.any(3).astype(int) + first.any(3).astype(int)


NEED = halo_need()


def plane_need(c, p):
    return NEED[c, p - LOW + 4].max()


def row_counts(c, p):
    need = NEED[c, p - LOW + 4]
    below, above = need[:4], need[4 + BX :]
    return tuple((int((side > 0).sum()), int((side > 1).sum())) for side in (below, above))


OWN = range(LOW, LOW + BX)
BELOW, ABOVE = 0, 1


def y_layout(side):
    at, rows = {}, 0
    for p in OWN:
        for field in range(6):
            count = row_counts(field % 3, p)[side][field // 3]
            at[p, field] = (rows, count)
            rows += count
    rows = -(-rows // 8) * 8
    for p in OWN[::2]:
        at[p, "packed"] = at[p + 1, "packed"] = rows
        rows += 4
    return at, rows


Y_LOW, Y_LOW_ROWS = y_layout(BELOW)
Y_HIGH, Y_HIGH_ROWS = y_layout(ABOVE)
Y_ROWS = -(-max(Y_LOW_ROWS, Y_HIGH_ROWS) // 8) * 8


def x_layout(planes):
    at, rows = {}, 0
    for p in planes:
        for field in range(6):
            if plane_need(field % 3, p) > field // 3:
                at[p, field] = rows
                rows += BY
    for p in planes:
        at[p, "packed"] = rows
        rows += 8
    for p in planes:
        at[p, "edge"] = rows
        rows += 4
    for p in planes:
        for field in range(6):
            for side in (BELOW, ABOVE):
                count = row_counts(field % 3, p)[side][field // 3]
                at[p, field, side] = (rows, count)
                rows += count
    return at, -(-rows // 8) * 8


X_LOW, X_LOW_ROWS = x_layout(range(LOW))
X_HIGH, X_HIGH_ROWS = x_layout(range(LOW + BX, EXT))


def call(body, out_shape, specs, scratch=(), flops=1000000):
    return pl.pallas_call(
        body,
        out_shape=out_shape,
        in_specs=specs,
        out_specs=jax.tree.map(lambda _: VMEM, out_shape),
        scratch_shapes=list(scratch),
        compiler_params=pltpu.CompilerParams(vmem_limit_bytes=VMEM_LIMIT),
        cost_estimate=pl.CostEstimate(flops=flops, bytes_accessed=1000000, transcendentals=0),
    )


def lanes(shape):
    return lax.broadcasted_iota(jnp.int32, shape, 1)


def rotate(v, shift, axis):
    return pltpu.roll(v, shift % v.shape[axis], axis)


def weigh(sigma):
    return jnp.where(sigma > 0.0, EDGE / (4.0 + sigma), 0.0)


def prepare(cond_in, rhs_in, fraction_in, region_in, flags_in, rhs, sigma, first_iter, packed_out, cond, fraction, region, flags, sems):
    copies = [
        pltpu.make_async_copy(source, target, sems.at[i])
        for i, (source, target) in enumerate(
            ((cond_in, cond), (region_in, region), (fraction_in, fraction), (flags_in, flags), (rhs_in, rhs))
        )
    ]
    for copy in copies:
        copy.start()
    for copy in copies:
        copy.wait()
    group = lanes((8, BZ)) // 8
    for x in range(BX):
        where = region[x]
        conductivity = jnp.full((BY, BZ), cond[0], jnp.float32)
        for number in range(1, 8):
            conductivity = jnp.where(where == number, cond[number], conductivity)
        packed = jnp.zeros((8, BZ), jnp.float32)
        for field in range(6):
            if field < 3:
                value = rhs[field, x]
            else:
                c = field - 3
                value = jnp.where(flags[c, x] == 0, conductivity * fraction[c, x], 0.0)
                sigma[c, x] = value
                first_iter[c, x] = weigh(value) * rhs[c, x]
            for tile in range(2):
                slot = field * 2 + tile
                moved = rotate(value[tile * 8 : tile * 8 + 8], LOW + 8 * slot, 1)
                packed = jnp.where(group == slot, moved, packed)
        packed_out[x] = packed


def send_y(ypar, rhs, sigma, first_iter, from_low, from_high, first_out, second_out, packed):
    below = (lanes((8, BZ)) % 8) < LOW
    odd = (lanes((4, BZ)) // 8) % 2
    for x in range(BX):
        packed[x] = jnp.where(below, from_low[x], from_high[x])

    def fill(out, layout, side):
        for p in OWN:
            for c in range(3):
                (at, count), (at_sigma, both) = layout[p, c], layout[p, c + 3]
                inner = 0 if side == ABOVE else BY - both
                outer = both if side == ABOVE else BY - count
                out[at_sigma : at_sigma + both] = sigma[c, p - LOW, inner : inner + both]
                place = at if side == ABOVE else at + count - both
                out[place : place + both] = rhs[c, p - LOW, inner : inner + both]
                place = at + both if side == ABOVE else at
                out[place : place + count - both] = first_iter[c, p - LOW, outer : outer + count - both]
        start = 0 if side == ABOVE else 4
        for p in OWN[::2]:
            value = packed[p - LOW, start : start + 4]
            other = packed[p + 1 - LOW, start : start + 4]
            at = layout[p, "packed"]
            out[at : at + 4] = jnp.where(odd == 1 - side, value, rotate(other, 8 if side == ABOVE else -8, 1))

    @pl.when(ypar[0] == 0)
    def _():
        fill(first_out, Y_LOW, BELOW)
        fill(second_out, Y_HIGH, ABOVE)

    @pl.when(ypar[0] != 0)
    def _():
        fill(second_out, Y_LOW, BELOW)
        fill(first_out, Y_HIGH, ABOVE)


def own_edge(p, y_low, y_high):
    odd = (lanes((4, BZ)) // 8) % 2 == 1
    above = y_high[Y_HIGH[p, "packed"] : Y_HIGH[p, "packed"] + 4]
    below = y_low[Y_LOW[p, "packed"] : Y_LOW[p, "packed"] + 4]
    if (p - LOW) % 2:
        above, below = rotate(above, -8, 1), rotate(below, 8, 1)
    return jnp.where(odd, below, above)


def send_x(ypar, rhs, sigma, first_iter, packed, first, second, up_out, down_out, y_low, y_high):
    even = ypar[0] == 0
    y_high[...] = jnp.where(even, first[1], second[1])
    y_low[...] = jnp.where(even, second[0], first[0])
    for out, layout, planes, step in (
        (up_out, X_LOW, range(LOW), BX),
        (down_out, X_HIGH, range(LOW + BX, EXT), -BX),
    ):
        for p in planes:
            own = p + step
            x = own - LOW
            at = layout[p, "packed"]
            out[at : at + 8] = packed[x]
            at = layout[p, "edge"]
            out[at : at + 4] = own_edge(own, y_low, y_high)
            for c in range(3):
                if plane_need(c, p) == 2:
                    at = layout[p, c]
                    out[at : at + BY] = rhs[c, x]
                    at = layout[p, c + 3]
                    out[at : at + BY] = sigma[c, x]
                elif plane_need(c, p) == 1:
                    at = layout[p, c]
                    out[at : at + BY] = first_iter[c, x]
                for side, source, have in ((BELOW, y_low, Y_LOW), (ABOVE, y_high, Y_HIGH)):
                    (at, count), (at_sigma, both) = layout[p, c, side], layout[p, c + 3, side]
                    (own_at, own_count), (own_sigma, own_both) = have[own, c], have[own, c + 3]

                    def rows(base, size, near, far):
                        return slice(base + near, base + far) if side == ABOVE else slice(base + size - far, base + size - near)

                    if both:
                        out[rows(at_sigma, both, 0, both)] = source[rows(own_sigma, own_both, 0, both)]
                        out[rows(at, count, 0, both)] = source[rows(own_at, own_count, 0, both)]
                    middle = min(max(both, own_both), count)
                    if both < middle:
                        out[rows(at, count, both, middle)] = (
                            weigh(source[rows(own_sigma, own_both, both, middle)])
                            * source[rows(own_at, own_count, both, middle)]
                        )
                    if middle < count:
                        out[rows(at, count, middle, count)] = source[rows(own_at, own_count, middle, count)]


def up_y(v):
    return rotate(v, -1, 0)


def down_y(v):
    return rotate(v, 1, 0)


def up_z(v):
    return rotate(v, -1, 1)


def down_z(v):
    return rotate(v, 1, 1)


def spread(p, main, halo, packed, edge, wide, weight, iterate):
    edge = jnp.concatenate([edge, rotate(edge, -8, 1)], axis=0)
    for field in range(6):
        need = plane_need(field % 3, p)
        if need == 0:
            continue
        target = wide(field, p)
        if need > field // 3:
            target[0:BY, 0:BZ] = main(field)
            rows = halo(field, ABOVE)
            if rows is not None:
                target[BY : BY + rows.shape[0], 0:BZ] = rows
            rows = halo(field, BELOW)
            if rows is not None:
                target[24 - rows.shape[0] : 24, 0:BZ] = rows
        target[0:8, BZ:] = rotate(packed, -(LOW + 16 * field), 1)
        target[8:16, BZ:] = rotate(packed, -(LOW + 16 * field + 8), 1)
        target[16:24, BZ:] = rotate(edge, -(LOW + 16 * field), 1)
    for c in range(3):
        need = plane_need(c, p)
        if need == 0:
            continue
        rhs, sigma, u = wide(c, p), wide(3 + c, p), iterate(c, p)
        if need == 1:
            u[:, 0:BZ] = rhs[:, 0:BZ]
            u[:, BZ:] = weigh(sigma[:, BZ:]) * rhs[:, BZ:]
            continue
        w = weigh(sigma[...])
        weight(c, p)[...] = w
        u[...] = w * rhs[...]
        (low_any, low_both), (high_any, high_both) = row_counts(c, p)
        for start, stop in ((BY + high_both, BY + high_any), (24 - low_any, 24 - low_both)):
            if start < stop:
                u[start:stop, 0:BZ] = rhs[start:stop, 0:BZ]


def faces(u, p):
    u0, u1, u2 = u(0, p)[...], u(1, p)[...], u(2, p)[...]
    f0 = (up_y(u2) - u2) - (up_z(u1) - u1)
    f1 = (up_z(u0) - u0) - (u(2, p + 1)[...] - u2)
    f2 = (u(1, p + 1)[...] - u1) - (up_y(u0) - u0)
    return f0, f1, f2


def curl0(f):
    return (down_z(f[1]) - f[1]) - (down_y(f[2]) - f[2])


def curl1(f, prev):
    return (prev[2] - f[2]) - (down_z(f[0]) - f[0])


def curl2(f, prev):
    return (down_y(f[0]) - f[0]) - (prev[1] - f[1])


def smooth(planes, wide, weight, iterate, second_iter):
    prev = faces(iterate, planes[0] - 1)
    for p in planes:
        f = faces(iterate, p)
        for c, k in enumerate((curl0(f), curl1(f, prev), curl2(f, prev))):
            u = iterate(c, p)[...]
            second_iter(c, p)[...] = u + weight(c, p)[...] * (wide(c, p)[...] - (k + wide(3 + c, p)[...] * u))
        prev = f


def restrict(planes, wide, second_iter, nodal):
    def residual(c, p, k):
        s = wide(3 + c, p)[...]
        return jnp.where(s > 0.0, wide(c, p)[...] - (k + s * second_iter(c, p)[...]), 0.0)

    prev = faces(second_iter, planes[0] - 1)
    before = residual(0, planes[0] - 1, curl0(prev))
    for p in planes:
        f = faces(second_iter, p)
        q0 = residual(0, p, curl0(f))
        q1 = residual(1, p, curl1(f, prev))
        q2 = residual(2, p, curl2(f, prev))
        d1, d2 = down_y(q1), down_z(q2)
        nodal(0, p)[...] = (before - q0) + (d1 - q1) + (d2 - q2)
        nodal(1, p)[...] = (before + q0) * 0.5
        nodal(2, p)[...] = (d1 + q1) * 0.5
        nodal(3, p)[...] = (d2 + q2) * 0.5
        prev, before = f, q0


INNER = {"wide": OWN, "weight": OWN, "iterate": OWN, "second": OWN[1:-1], "nodal": OWN[2:-2]}
USED = {"wide": range(EXT), "weight": range(EXT), "iterate": range(EXT), "second": range(1, EXT - 1), "nodal": range(2, EXT - 2)}
OUTER = {name: [p for p in USED[name] if p not in INNER[name]] for name in USED}
FIELDS = {"wide": 6, "weight": 3, "iterate": 3, "second": 3, "nodal": 4}


def plane_arrays(kind, inner, outer=None):
    at = {p: (inner, i) for i, p in enumerate(INNER[kind])}
    if outer is not None:
        at.update({p: (outer, i) for i, p in enumerate(OUTER[kind])})
    return lambda c, p: at[p][0].at[c, at[p][1]]


def stencil_inner(rhs, sigma, packed, y_low, y_high, *arrays):
    wide, weight, iterate, second_iter, nodal = (plane_arrays(k, ref) for k, ref in zip(FIELDS, arrays))
    for p in OWN:

        def main(field):
            return (rhs if field < 3 else sigma)[field % 3, p - LOW]

        def halo(field, side):
            at, count = (Y_LOW, Y_HIGH)[side][p, field]
            return (y_low, y_high)[side][at : at + count] if count else None

        spread(p, main, halo, packed[p - LOW], own_edge(p, y_low, y_high), wide, weight, iterate)
    smooth(INNER["second"], wide, weight, iterate, second_iter)
    restrict(INNER["nodal"], wide, second_iter, nodal)


def stencil_outer(rhs, sigma, low, high, *arrays):
    inner, out, outer = arrays[:5], arrays[5], arrays[6:]
    wide, weight, iterate, second_iter, nodal = (plane_arrays(k, *refs) for k, refs in zip(FIELDS, zip(inner, outer)))
    for p in OUTER["wide"]:
        ref, layout = (low, X_LOW) if p < LOW else (high, X_HIGH)

        def main(field):
            return ref[layout[p, field] : layout[p, field] + BY]

        def halo(field, side):
            at, count = layout[p, field, side]
            return ref[at : at + count] if count else None

        packed, edge = layout[p, "packed"], layout[p, "edge"]
        spread(p, main, halo, ref[packed : packed + 8], ref[edge : edge + 4], wide, weight, iterate)
    smooth([p for p in OUTER["second"] if p < LOW + 2], wide, weight, iterate, second_iter)
    smooth([p for p in OUTER["second"] if p > LOW + 2], wide, weight, iterate, second_iter)
    restrict([p for p in OUTER["nodal"] if p < LOW + 3], wide, second_iter, nodal)
    restrict([p for p in OUTER["nodal"] if p > LOW + 3], wide, second_iter, nodal)

    def node(c, p):
        b = nodal(c, p)[...]
        near = (nodal(c, p - 1)[...] + nodal(c, p + 1)[...]) + (up_y(b) + down_y(b)) + (up_z(b) + down_z(b))
        return (1.2 * NODE) * b + (NODE * NODE) * near

    n0, n1 = node(0, LOW), node(1, LOW)
    for x in range(BX):
        p = x + LOW
        n0_next, n1_next = node(0, p + 1), node(1, p + 1)
        n2, n3 = node(2, p), node(3, p)
        corrections = (
            (n0_next - n0) + (n1_next + n1) * 0.5,
            (up_y(n0) - n0) + (n2 + up_y(n2)) * 0.5,
            (up_z(n0) - n0) + (n3 + up_z(n3)) * 0.5,
        )
        for c in range(3):
            kept = second_iter(c, p)[0:BY, 0:BZ] + corrections[c][0:BY, 0:BZ]
            out[c, x] = jnp.where(sigma[c, x] > 0.0, kept, 0.96 * rhs[c, x])
        n0, n1 = n0_next, n1_next


def pairs(count):
    return (
        [[i, i + 1] for i in range(0, count, 2)],
        [[i, (i + 1) % count] for i in range(1, count, 2)],
    )


def gather(value, axis, groups):
    return lax.all_gather(value, axis, axis=0, tiled=False, axis_index_groups=groups)


def shift(value, axis, step):
    count = lax.axis_size(axis)
    return lax.ppermute(value, axis, [(i, (i + step) % count) for i in range(count)])


def on_device(rhs, conductivity, fraction, region, flags):
    f32 = functools.partial(jax.ShapeDtypeStruct, dtype=jnp.float32)
    ypar = (lax.axis_index("gy") & 1).astype(jnp.int32).reshape(1)

    block = f32((3, BX, BY, BZ))
    lane_block = f32((BX, 8, BZ))
    rhs, sigma, first_iter, packed = call(
        prepare,
        (block, block, block, lane_block),
        [HBM] * 5,
        scratch=(
            pltpu.SMEM((8,), jnp.float32),
            pltpu.VMEM((3, BX, BY, BZ), jnp.float32),
            pltpu.VMEM((BX, BY, BZ), jnp.int32),
            pltpu.VMEM((3, BX, BY, BZ), jnp.int32),
            pltpu.SemaphoreType.DMA((5,)),
        ),
    )(*(pltpu.with_memory_space_constraint(a, pltpu.HBM) for a in (conductivity, rhs, fraction, region, flags)))

    from_low = shift(packed, "gz", 1)
    from_high = shift(packed, "gz", -1)

    even_y, odd_y = pairs(lax.axis_size("gy"))
    payload = f32((Y_ROWS, BZ))
    to_first, to_second, packed = call(
        send_y, (payload, payload, lane_block), [SMEM] + [VMEM] * 5
    )(ypar, rhs, sigma, first_iter, from_low, from_high)
    first = gather(to_first, "gy", even_y)
    second = gather(to_second, "gy", odd_y)

    up, down, y_low, y_high = call(
        send_x, (f32((X_LOW_ROWS, BZ)), f32((X_HIGH_ROWS, BZ)), payload, payload), [SMEM] + [VMEM] * 6
    )(ypar, rhs, sigma, first_iter, packed, first, second)
    low = shift(up, "gx", 1)
    high = shift(down, "gx", -1)

    inner = call(
        stencil_inner,
        tuple(f32((FIELDS[kind], len(INNER[kind]), 24, 2 * BZ)) for kind in FIELDS),
        [VMEM] * 5,
        flops=20000000,
    )(rhs, sigma, packed, y_low, y_high)
    return call(
        stencil_outer,
        block,
        [VMEM] * 9,
        scratch=[pltpu.VMEM((FIELDS[kind], len(OUTER[kind]), 24, 2 * BZ), jnp.float32) for kind in FIELDS],
    )(rhs, sigma, low, high, *inner)


def solution(mesh):
    return jax.shard_map(
        on_device,
        mesh=mesh,
        in_specs=(
            P(None, "gx", "gy", "gz"),
            P(),
            P(None, "gx", "gy", "gz"),
            P("gx", "gy", "gz"),
            P(None, "gx", "gy", "gz"),
        ),
        out_specs=P(None, "gx", "gy", "gz"),
        check_vma=False,
    )
```

```python
import functools

import jax
import jax.numpy as jnp
import numpy as np
from jax import lax
from jax.experimental import pallas as pl
from jax.experimental.pallas import tpu as pltpu
from jax.sharding import PartitionSpec as P


EDGE = 0.8
NODE = 0.8 / 7.0

BX, BY, BZ = 8, 16, 128
LOW, HIGH = 3, 4
EXT = LOW + BX + HIGH
VMEM_LIMIT = 16 * 1024 * 1024

VMEM = pl.BlockSpec(memory_space=pltpu.VMEM)
SMEM = pl.BlockSpec(memory_space=pltpu.SMEM)
HBM = pl.BlockSpec(memory_space=pltpu.HBM)


def halo_need():
    size = BX + 9

    def at(need, axis, k):
        return np.roll(need, k, axis)

    out = np.zeros((3, size, size, size), bool)
    out[:, 4 : 4 + BX, 4 : 4 + BX, 4 : 4 + BX] = True
    node = np.zeros((4, size, size, size), bool)
    for a in range(3):
        both = out[a] | at(out[a], a, 1)
        node[0] |= both
        node[a + 1] |= both
    near = node.copy()
    for a in range(3):
        near |= np.roll(node, 1, a + 1) | np.roll(node, -1, a + 1)
    masked = np.stack([near[0] | at(near[0], a, -1) | near[a + 1] | at(near[a + 1], a, -1) for a in range(3)])

    def operand(need):
        face = np.zeros_like(need)
        for a in range(3):
            b, c = (a + 1) % 3, (a + 2) % 3
            face[b] |= need[a] | at(need[a], c, -1)
            face[c] |= need[a] | at(need[a], b, -1)
        edge = need.copy()
        for a in range(3):
            b, c = (a + 1) % 3, (a + 2) % 3
            edge[b] |= face[a] | at(face[a], c, 1)
            edge[c] |= face[a] | at(face[a], b, 1)
        return edge

    second = operand(masked) | out
    first = operand(second)
    return second.any(3).astype(int) + first.any(3).astype(int)


NEED = halo_need()


def plane_need(c, p):
    return NEED[c, p - LOW + 4].max()


def row_counts(c, p):
    need = NEED[c, p - LOW + 4]
    below, above = need[:4], need[4 + BX :]
    return tuple((int((side > 0).sum()), int((side > 1).sum())) for side in (below, above))


OWN = range(LOW, LOW + BX)
BELOW, ABOVE = 0, 1


def y_layout(side):
    at, rows = {}, 0
    for p in OWN:
        for field in range(6):
            count = row_counts(field % 3, p)[side][field // 3]
            at[p, field] = (rows, count)
            rows += count
    rows = -(-rows // 8) * 8
    for p in OWN[::2]:
        at[p, "packed"] = at[p + 1, "packed"] = rows
        rows += 4
    return at, rows


Y_LOW, Y_LOW_ROWS = y_layout(BELOW)
Y_HIGH, Y_HIGH_ROWS = y_layout(ABOVE)
Y_ROWS = -(-max(Y_LOW_ROWS, Y_HIGH_ROWS) // 8) * 8


def x_layout(planes):
    at, rows = {}, 0
    for p in planes:
        for field in range(6):
            if plane_need(field % 3, p) > field // 3:
                at[p, field] = rows
                rows += BY
    for p in planes:
        at[p, "packed"] = rows
        rows += 8
    for p in planes:
        at[p, "edge"] = rows
        rows += 4
    for p in planes:
        for field in range(6):
            for side in (BELOW, ABOVE):
                count = row_counts(field % 3, p)[side][field // 3]
                at[p, field, side] = (rows, count)
                rows += count
    return at, -(-rows // 8) * 8


X_LOW, X_LOW_ROWS = x_layout(range(LOW))
X_HIGH, X_HIGH_ROWS = x_layout(range(LOW + BX, EXT))


def call(body, out_shape, specs, scratch=(), flops=1000000):
    return pl.pallas_call(
        body,
        out_shape=out_shape,
        in_specs=specs,
        out_specs=jax.tree.map(lambda _: VMEM, out_shape),
        scratch_shapes=list(scratch),
        compiler_params=pltpu.CompilerParams(vmem_limit_bytes=VMEM_LIMIT),
        cost_estimate=pl.CostEstimate(flops=flops, bytes_accessed=1000000, transcendentals=0),
    )


def lanes(shape):
    return lax.broadcasted_iota(jnp.int32, shape, 1)


def rotate(v, shift, axis):
    return pltpu.roll(v, shift % v.shape[axis], axis)


def weigh(sigma):
    return jnp.where(sigma > 0.0, EDGE / (4.0 + sigma), 0.0)


def prepare(cond_in, rhs_in, fraction_in, region_in, flags_in, rhs, sigma, first_iter, packed_out, cond, fraction, region, flags, sems):
    copies = [
        pltpu.make_async_copy(source, target, sems.at[i])
        for i, (source, target) in enumerate(
            ((cond_in, cond), (region_in, region), (fraction_in, fraction), (flags_in, flags), (rhs_in, rhs))
        )
    ]
    for copy in copies:
        copy.start()
    for copy in copies:
        copy.wait()
    group = lanes((8, BZ)) // 8
    for x in range(BX):
        where = region[x]
        conductivity = jnp.full((BY, BZ), cond[0], jnp.float32)
        for number in range(1, 8):
            conductivity = jnp.where(where == number, cond[number], conductivity)
        packed = jnp.zeros((8, BZ), jnp.float32)
        for field in range(6):
            if field < 3:
                value = rhs[field, x]
            else:
                c = field - 3
                value = jnp.where(flags[c, x] == 0, conductivity * fraction[c, x], 0.0)
                sigma[c, x] = value
                first_iter[c, x] = weigh(value) * rhs[c, x]
            for tile in range(2):
                slot = field * 2 + tile
                moved = rotate(value[tile * 8 : tile * 8 + 8], LOW + 8 * slot, 1)
                packed = jnp.where(group == slot, moved, packed)
        packed_out[x] = packed


def send_y(ypar, rhs, sigma, first_iter, from_low, from_high, first_out, second_out, packed):
    below = (lanes((8, BZ)) % 8) < LOW
    odd = (lanes((4, BZ)) // 8) % 2
    for x in range(BX):
        packed[x] = jnp.where(below, from_low[x], from_high[x])

    def fill(out, layout, side):
        for p in OWN:
            for c in range(3):
                (at, count), (at_sigma, both) = layout[p, c], layout[p, c + 3]
                inner = 0 if side == ABOVE else BY - both
                outer = both if side == ABOVE else BY - count
                out[at_sigma : at_sigma + both] = sigma[c, p - LOW, inner : inner + both]
                place = at if side == ABOVE else at + count - both
                out[place : place + both] = rhs[c, p - LOW, inner : inner + both]
                place = at + both if side == ABOVE else at
                out[place : place + count - both] = first_iter[c, p - LOW, outer : outer + count - both]
        start = 0 if side == ABOVE else 4
        for p in OWN[::2]:
            value = packed[p - LOW, start : start + 4]
            other = packed[p + 1 - LOW, start : start + 4]
            at = layout[p, "packed"]
            out[at : at + 4] = jnp.where(odd == 1 - side, value, rotate(other, 8 if side == ABOVE else -8, 1))

    @pl.when(ypar[0] == 0)
    def _():
        fill(first_out, Y_LOW, BELOW)
        fill(second_out, Y_HIGH, ABOVE)

    @pl.when(ypar[0] != 0)
    def _():
        fill(second_out, Y_LOW, BELOW)
        fill(first_out, Y_HIGH, ABOVE)


def own_edge(p, y_low, y_high):
    odd = (lanes((4, BZ)) // 8) % 2 == 1
    above = y_high[Y_HIGH[p, "packed"] : Y_HIGH[p, "packed"] + 4]
    below = y_low[Y_LOW[p, "packed"] : Y_LOW[p, "packed"] + 4]
    if (p - LOW) % 2:
        above, below = rotate(above, -8, 1), rotate(below, 8, 1)
    return jnp.where(odd, below, above)


def send_x(ypar, rhs, sigma, first_iter, packed, first, second, up_out, down_out, y_low, y_high):
    even = ypar[0] == 0
    y_high[...] = jnp.where(even, first[1], second[1])
    y_low[...] = jnp.where(even, second[0], first[0])
    for out, layout, planes, step in (
        (up_out, X_LOW, range(LOW), BX),
        (down_out, X_HIGH, range(LOW + BX, EXT), -BX),
    ):
        for p in planes:
            own = p + step
            x = own - LOW
            at = layout[p, "packed"]
            out[at : at + 8] = packed[x]
            at = layout[p, "edge"]
            out[at : at + 4] = own_edge(own, y_low, y_high)
            for c in range(3):
                if plane_need(c, p) == 2:
                    at = layout[p, c]
                    out[at : at + BY] = rhs[c, x]
                    at = layout[p, c + 3]
                    out[at : at + BY] = sigma[c, x]
                elif plane_need(c, p) == 1:
                    at = layout[p, c]
                    out[at : at + BY] = first_iter[c, x]
                for side, source, have in ((BELOW, y_low, Y_LOW), (ABOVE, y_high, Y_HIGH)):
                    (at, count), (at_sigma, both) = layout[p, c, side], layout[p, c + 3, side]
                    (own_at, own_count), (own_sigma, own_both) = have[own, c], have[own, c + 3]

                    def rows(base, size, near, far):
                        return slice(base + near, base + far) if side == ABOVE else slice(base + size - far, base + size - near)

                    if both:
                        out[rows(at_sigma, both, 0, both)] = source[rows(own_sigma, own_both, 0, both)]
                        out[rows(at, count, 0, both)] = source[rows(own_at, own_count, 0, both)]
                    middle = min(max(both, own_both), count)
                    if both < middle:
                        out[rows(at, count, both, middle)] = (
                            weigh(source[rows(own_sigma, own_both, both, middle)])
                            * source[rows(own_at, own_count, both, middle)]
                        )
                    if middle < count:
                        out[rows(at, count, middle, count)] = source[rows(own_at, own_count, middle, count)]


def up_y(v):
    return rotate(v, -1, 0)


def down_y(v):
    return rotate(v, 1, 0)


def up_z(v):
    return rotate(v, -1, 1)


def down_z(v):
    return rotate(v, 1, 1)


def spread(p, main, halo, packed, edge, wide, weight, iterate):
    edge = jnp.concatenate([edge, rotate(edge, -8, 1)], axis=0)
    for field in range(6):
        need = plane_need(field % 3, p)
        if need == 0:
            continue
        target = wide(field, p)
        if need > field // 3:
            target[0:BY, 0:BZ] = main(field)
            rows = halo(field, ABOVE)
            if rows is not None:
                target[BY : BY + rows.shape[0], 0:BZ] = rows
            rows = halo(field, BELOW)
            if rows is not None:
                target[24 - rows.shape[0] : 24, 0:BZ] = rows
        target[0:8, BZ:] = rotate(packed, -(LOW + 16 * field), 1)
        target[8:16, BZ:] = rotate(packed, -(LOW + 16 * field + 8), 1)
        target[16:24, BZ:] = rotate(edge, -(LOW + 16 * field), 1)
    for c in range(3):
        need = plane_need(c, p)
        if need == 0:
            continue
        rhs, sigma, u = wide(c, p), wide(3 + c, p), iterate(c, p)
        if need == 1:
            u[:, 0:BZ] = rhs[:, 0:BZ]
            u[:, BZ:] = weigh(sigma[:, BZ:]) * rhs[:, BZ:]
            continue
        w = weigh(sigma[...])
        weight(c, p)[...] = w
        u[...] = w * rhs[...]
        (low_any, low_both), (high_any, high_both) = row_counts(c, p)
        for start, stop in ((BY + high_both, BY + high_any), (24 - low_any, 24 - low_both)):
            if start < stop:
                u[start:stop, 0:BZ] = rhs[start:stop, 0:BZ]


def faces(u, p):
    u0, u1, u2 = u(0, p)[...], u(1, p)[...], u(2, p)[...]
    f0 = (up_y(u2) - u2) - (up_z(u1) - u1)
    f1 = (up_z(u0) - u0) - (u(2, p + 1)[...] - u2)
    f2 = (u(1, p + 1)[...] - u1) - (up_y(u0) - u0)
    return f0, f1, f2


def curl0(f):
    return (down_z(f[1]) - f[1]) - (down_y(f[2]) - f[2])


def curl1(f, prev):
    return (prev[2] - f[2]) - (down_z(f[0]) - f[0])


def curl2(f, prev):
    return (down_y(f[0]) - f[0]) - (prev[1] - f[1])


def update(c, p, k, wide, weight, iterate):
    u = iterate(c, p)[...]
    return u + weight(c, p)[...] * (wide(c, p)[...] - (k + wide(3 + c, p)[...] * u))


def smooth(planes, prev, wide, weight, iterate, second_iter):
    for p in planes:
        f = faces(iterate, p)
        for c, k in enumerate((curl0(f), curl1(f, prev), curl2(f, prev))):
            second_iter(c, p)[...] = update(c, p, k, wide, weight, iterate)
        prev = f
    return prev


def defect(c, p, k, wide, second_iter):
    return wide(c, p)[...] - (k + wide(3 + c, p)[...] * second_iter(c, p)[...])


def kept(c, p, value, wide):
    return jnp.where(wide(3 + c, p)[...] > 0.0, value, 0.0)


def gather_nodes(p, before, q0, q1, q2, nodal):
    d1, d2 = down_y(q1), down_z(q2)
    nodal(0, p)[...] = (before - q0) + (d1 - q1) + (d2 - q2)
    nodal(1, p)[...] = (before + q0) * 0.5
    nodal(2, p)[...] = (d1 + q1) * 0.5
    nodal(3, p)[...] = (d2 + q2) * 0.5


def restrict(planes, prev, before, wide, second_iter, nodal):
    for p in planes:
        f = faces(second_iter, p)
        q = [
            kept(c, p, defect(c, p, k, wide, second_iter), wide)
            for c, k in enumerate((curl0(f), curl1(f, prev), curl2(f, prev)))
        ]
        gather_nodes(p, before, *q, nodal)
        prev, before = f, q[0]
    return prev, before


def beside(c, p, nodal):
    b = nodal(c, p)[...]
    return (1.2 * NODE) * b + (NODE * NODE) * ((up_y(b) + down_y(b)) + (up_z(b) + down_z(b)))


def finish(p, n0, n0_next, n1, n1_next, n2, n3, second_iter, rhs, sigma):
    corrections = (
        (n0_next - n0) + (n1_next + n1) * 0.5,
        (up_y(n0) - n0) + (n2 + up_y(n2)) * 0.5,
        (up_z(n0) - n0) + (n3 + up_z(n3)) * 0.5,
    )
    return [
        jnp.where(
            sigma[c, p - LOW] > 0.0,
            second_iter(c, p)[0:BY, 0:BZ] + corrections[c][0:BY, 0:BZ],
            0.96 * rhs[c, p - LOW],
        )
        for c in range(3)
    ]


INNER = {"wide": OWN, "weight": OWN, "iterate": OWN, "second": OWN[1:-1], "nodal": OWN[2:-2]}
USED = {"wide": range(EXT), "weight": range(EXT), "iterate": range(EXT), "second": range(1, EXT - 1), "nodal": range(2, EXT - 2)}
OUTER = {name: [p for p in USED[name] if p not in INNER[name]] for name in USED}
INNER |= {"second_part": OWN[:1], "second_carry": OWN[-2:-1], "nodal_part": OWN[1:2], "nodal_carry": OWN[-3:-2], "beside": OWN[2:-2]}
FIELDS = {
    "wide": 6, "weight": 3, "iterate": 3, "second": 3, "nodal": 4,
    "second_part": 3, "second_carry": 2, "nodal_part": 3, "nodal_carry": 3, "beside": 4,
}
MIDDLE = OWN[3]


def plane_arrays(kind, inner, outer=None):
    at = {p: (inner, i) for i, p in enumerate(INNER[kind])}
    if outer is not None:
        at.update({p: (outer, i) for i, p in enumerate(OUTER[kind])})
    return lambda c, p: at[p][0].at[c, at[p][1]]


def stencil_inner(rhs, sigma, packed, y_low, y_high, middle, *arrays):
    wide, weight, iterate, second_iter, nodal, second_part, second_carry, nodal_part, nodal_carry, near = (
        plane_arrays(kind, ref) for kind, ref in zip(FIELDS, arrays)
    )
    for p in OWN:

        def main(field):
            return (rhs if field < 3 else sigma)[field % 3, p - LOW]

        def halo(field, side):
            at, count = (Y_LOW, Y_HIGH)[side][p, field]
            return (y_low, y_high)[side][at : at + count] if count else None

        spread(p, main, halo, packed[p - LOW], own_edge(p, y_low, y_high), wide, weight, iterate)

    p = OWN[0]
    prev = f = faces(iterate, p)
    k = (curl0(f), -f[2] - (down_z(f[0]) - f[0]), (down_y(f[0]) - f[0]) + f[1])
    for c in range(3):
        second_part(c, p)[...] = update(c, p, k[c], wide, weight, iterate)
    prev = smooth(INNER["second"], prev, wide, weight, iterate, second_iter)
    for i in range(2):
        second_carry(i, INNER["second"][-1])[...] = prev[1 + i]

    p = OWN[1]
    prev = f = faces(second_iter, p)
    before = kept(0, p, defect(0, p, curl0(f), wide, second_iter), wide)
    nodal_part(0, p)[...] = before
    nodal_part(1, p)[...] = defect(1, p, -f[2] - (down_z(f[0]) - f[0]), wide, second_iter)
    nodal_part(2, p)[...] = defect(2, p, (down_y(f[0]) - f[0]) + f[1], wide, second_iter)
    prev, before = restrict(INNER["nodal"], prev, before, wide, second_iter, nodal)
    for i, value in enumerate((prev[1], prev[2], before)):
        nodal_carry(i, INNER["nodal"][-1])[...] = value

    for p in INNER["beside"]:
        for c in range(4):
            near(c, p)[...] = beside(c, p, nodal)

    def node(c, p):
        return near(c, p)[...] + (NODE * NODE) * (nodal(c, p - 1)[...] + nodal(c, p + 1)[...])

    p = MIDDLE
    planes = finish(
        p, node(0, p), node(0, p + 1), node(1, p), node(1, p + 1), node(2, p), node(3, p), second_iter, rhs, sigma
    )
    for c in range(3):
        middle[c] = planes[c]


def stencil_outer(rhs, sigma, low, high, middle, *arrays):
    inner, out, outer = arrays[: len(FIELDS)], arrays[len(FIELDS)], arrays[len(FIELDS) + 1 :]
    wide, weight, iterate, second_iter, nodal = (plane_arrays(k, *refs) for k, refs in zip(FIELDS, zip(inner, outer)))
    second_part, second_carry, nodal_part, nodal_carry, near = (
        plane_arrays(kind, ref) for kind, ref in list(zip(FIELDS, inner))[5:]
    )
    for p in OUTER["wide"]:
        ref, layout = (low, X_LOW) if p < LOW else (high, X_HIGH)

        def main(field):
            return ref[layout[p, field] : layout[p, field] + BY]

        def halo(field, side):
            at, count = layout[p, field, side]
            return ref[at : at + count] if count else None

        packed, edge = layout[p, "packed"], layout[p, "edge"]
        spread(p, main, halo, ref[packed : packed + 8], ref[edge : edge + 4], wide, weight, iterate)

    first, last = INNER["second"][0] - 1, INNER["second"][-1]
    prev = smooth(range(1, first), faces(iterate, 0), wide, weight, iterate, second_iter)
    second_iter(0, first)[...] = second_part(0, first)[...]
    second_iter(1, first)[...] = second_part(1, first)[...] - weight(1, first)[...] * prev[2]
    second_iter(2, first)[...] = second_part(2, first)[...] + weight(2, first)[...] * prev[1]
    prev = (None, second_carry(0, last)[...], second_carry(1, last)[...])
    smooth(range(last + 1, EXT - 1), prev, wide, weight, iterate, second_iter)

    first, last = INNER["nodal"][0] - 1, INNER["nodal"][-1]
    prev = faces(second_iter, 1)
    before = kept(0, 1, defect(0, 1, curl0(prev), wide, second_iter), wide)
    prev, before = restrict(range(2, first), prev, before, wide, second_iter, nodal)
    q1 = kept(1, first, nodal_part(1, first)[...] - prev[2], wide)
    q2 = kept(2, first, nodal_part(2, first)[...] + prev[1], wide)
    gather_nodes(first, before, nodal_part(0, first)[...], q1, q2, nodal)
    prev = (None, nodal_carry(0, last)[...], nodal_carry(1, last)[...])
    restrict(range(last + 1, EXT - 2), prev, nodal_carry(2, last)[...], wide, second_iter, nodal)

    def node(c, p):
        own = near(c, p)[...] if p in INNER["beside"] else beside(c, p, nodal)
        return own + (NODE * NODE) * (nodal(c, p - 1)[...] + nodal(c, p + 1)[...])

    n0, n1 = node(0, LOW), node(1, LOW)
    for p in OWN:
        n0_next, n1_next = node(0, p + 1), node(1, p + 1)
        if p == MIDDLE:
            planes = [middle[c] for c in range(3)]
        else:
            planes = finish(p, n0, n0_next, n1, n1_next, node(2, p), node(3, p), second_iter, rhs, sigma)
        for c in range(3):
            out[c, p - LOW] = planes[c]
        n0, n1 = n0_next, n1_next


def pairs(count):
    return (
        [[i, i + 1] for i in range(0, count, 2)],
        [[i, (i + 1) % count] for i in range(1, count, 2)],
    )


def gather(value, axis, groups):
    return lax.all_gather(value, axis, axis=0, tiled=False, axis_index_groups=groups)


def shift(value, axis, step):
    count = lax.axis_size(axis)
    return lax.ppermute(value, axis, [(i, (i + step) % count) for i in range(count)])


def on_device(rhs, conductivity, fraction, region, flags):
    f32 = functools.partial(jax.ShapeDtypeStruct, dtype=jnp.float32)
    ypar = (lax.axis_index("gy") & 1).astype(jnp.int32).reshape(1)

    block = f32((3, BX, BY, BZ))
    lane_block = f32((BX, 8, BZ))
    rhs, sigma, first_iter, packed = call(
        prepare,
        (block, block, block, lane_block),
        [HBM] * 5,
        scratch=(
            pltpu.SMEM((8,), jnp.float32),
            pltpu.VMEM((3, BX, BY, BZ), jnp.float32),
            pltpu.VMEM((BX, BY, BZ), jnp.int32),
            pltpu.VMEM((3, BX, BY, BZ), jnp.int32),
            pltpu.SemaphoreType.DMA((5,)),
        ),
    )(*(pltpu.with_memory_space_constraint(a, pltpu.HBM) for a in (conductivity, rhs, fraction, region, flags)))

    from_low = shift(packed, "gz", 1)
    from_high = shift(packed, "gz", -1)

    even_y, odd_y = pairs(lax.axis_size("gy"))
    payload = f32((Y_ROWS, BZ))
    to_first, to_second, packed = call(
        send_y, (payload, payload, lane_block), [SMEM] + [VMEM] * 5
    )(ypar, rhs, sigma, first_iter, from_low, from_high)
    first = gather(to_first, "gy", even_y)
    second = gather(to_second, "gy", odd_y)

    up, down, y_low, y_high = call(
        send_x, (f32((X_LOW_ROWS, BZ)), f32((X_HIGH_ROWS, BZ)), payload, payload), [SMEM] + [VMEM] * 6
    )(ypar, rhs, sigma, first_iter, packed, first, second)
    low = shift(up, "gx", 1)
    high = shift(down, "gx", -1)

    inner = call(
        stencil_inner,
        (f32((3, BY, BZ)), *(f32((FIELDS[kind], len(INNER[kind]), 24, 2 * BZ)) for kind in FIELDS)),
        [VMEM] * 5,
        flops=20000000,
    )(rhs, sigma, packed, y_low, y_high)
    return call(
        stencil_outer,
        block,
        [VMEM] * (5 + len(FIELDS)),
        scratch=[pltpu.VMEM((FIELDS[kind], len(OUTER[kind]), 24, 2 * BZ), jnp.float32) for kind in OUTER],
    )(rhs, sigma, low, high, *inner)


def solution(mesh):
    return jax.shard_map(
        on_device,
        mesh=mesh,
        in_specs=(
            P(None, "gx", "gy", "gz"),
            P(),
            P(None, "gx", "gy", "gz"),
            P("gx", "gy", "gz"),
            P(None, "gx", "gy", "gz"),
        ),
        out_specs=P(None, "gx", "gy", "gz"),
        check_vma=False,
    )
```

```python
import functools

import jax
import jax.numpy as jnp
import numpy as np
from jax import lax
from jax.experimental import pallas as pl
from jax.experimental.pallas import tpu as pltpu
from jax.sharding import PartitionSpec as P


EDGE = 0.8
NODE = 0.8 / 7.0

BX, BY, BZ = 8, 16, 128
LOW, HIGH = 3, 4
EXT = LOW + BX + HIGH
VMEM_LIMIT = 16 * 1024 * 1024

VMEM = pl.BlockSpec(memory_space=pltpu.VMEM)
SMEM = pl.BlockSpec(memory_space=pltpu.SMEM)
HBM = pl.BlockSpec(memory_space=pltpu.HBM)


def halo_need():
    size = BX + 9

    def at(need, axis, k):
        return np.roll(need, k, axis)

    out = np.zeros((3, size, size, size), bool)
    out[:, 4 : 4 + BX, 4 : 4 + BX, 4 : 4 + BX] = True
    node = np.zeros((4, size, size, size), bool)
    for a in range(3):
        both = out[a] | at(out[a], a, 1)
        node[0] |= both
        node[a + 1] |= both
    near = node.copy()
    for a in range(3):
        near |= np.roll(node, 1, a + 1) | np.roll(node, -1, a + 1)
    masked = np.stack([near[0] | at(near[0], a, -1) | near[a + 1] | at(near[a + 1], a, -1) for a in range(3)])

    def operand(need):
        face = np.zeros_like(need)
        for a in range(3):
            b, c = (a + 1) % 3, (a + 2) % 3
            face[b] |= need[a] | at(need[a], c, -1)
            face[c] |= need[a] | at(need[a], b, -1)
        edge = need.copy()
        for a in range(3):
            b, c = (a + 1) % 3, (a + 2) % 3
            edge[b] |= face[a] | at(face[a], c, 1)
            edge[c] |= face[a] | at(face[a], b, 1)
        return edge

    second = operand(masked) | out
    first = operand(second)
    return second.any(3).astype(int) + first.any(3).astype(int)


NEED = halo_need()


def plane_need(c, p):
    return NEED[c, p - LOW + 4].max()


def row_counts(c, p):
    need = NEED[c, p - LOW + 4]
    below, above = need[:4], need[4 + BX :]
    return tuple((int((side > 0).sum()), int((side > 1).sum())) for side in (below, above))


OWN = range(LOW, LOW + BX)
BELOW, ABOVE = 0, 1


def y_layout(side):
    at, rows = {}, 0
    for p in OWN:
        for field in range(6):
            count = row_counts(field % 3, p)[side][field // 3]
            at[p, field] = (rows, count)
            rows += count
    rows = -(-rows // 8) * 8
    for p in OWN[::2]:
        at[p, "packed"] = at[p + 1, "packed"] = rows
        rows += 4
    return at, rows


Y_LOW, Y_LOW_ROWS = y_layout(BELOW)
Y_HIGH, Y_HIGH_ROWS = y_layout(ABOVE)
Y_ROWS = -(-max(Y_LOW_ROWS, Y_HIGH_ROWS) // 8) * 8


def x_layout(planes):
    at, rows = {}, 0
    for p in planes:
        for field in range(6):
            if plane_need(field % 3, p) > field // 3:
                at[p, field] = rows
                rows += BY
    for p in planes:
        for field in range(6):
            for side in (BELOW, ABOVE):
                count = row_counts(field % 3, p)[side][field // 3]
                at[p, field, side] = (rows, count)
                rows += count
    rows = -(-rows // 4) * 4
    for p in planes:
        at[p, "edge"] = rows
        rows += 4
    rows = -(-rows // 8) * 8
    for p in planes:
        at[p, "packed"] = rows
        rows += 8
    return at, -(-rows // 8) * 8


X_LOW, X_LOW_ROWS = x_layout(range(LOW))
X_HIGH, X_HIGH_ROWS = x_layout(range(LOW + BX, EXT))


def call(body, out_shape, specs, scratch=(), flops=1000000):
    return pl.pallas_call(
        body,
        out_shape=out_shape,
        in_specs=specs,
        out_specs=jax.tree.map(lambda _: VMEM, out_shape),
        scratch_shapes=list(scratch),
        compiler_params=pltpu.CompilerParams(vmem_limit_bytes=VMEM_LIMIT),
        cost_estimate=pl.CostEstimate(flops=flops, bytes_accessed=1000000, transcendentals=0),
    )


def lanes(shape):
    return lax.broadcasted_iota(jnp.int32, shape, 1)


def rotate(v, shift, axis):
    return pltpu.roll(v, shift % v.shape[axis], axis)


def weigh(sigma):
    return jnp.where(sigma > 0.0, EDGE / (4.0 + sigma), 0.0)


def prepare(cond_in, rhs_in, fraction_in, region_in, flags_in, rhs, sigma, first_iter, packed_out, cond, fraction, region, flags, sems):
    copies = [
        pltpu.make_async_copy(source, target, sems.at[i])
        for i, (source, target) in enumerate(
            ((cond_in, cond), (region_in, region), (fraction_in, fraction), (flags_in, flags), (rhs_in, rhs))
        )
    ]
    for copy in copies:
        copy.start()
    for copy in copies:
        copy.wait()
    group = lanes((8, BZ)) // 8
    for x in range(BX):
        where = region[x]
        conductivity = jnp.full((BY, BZ), cond[0], jnp.float32)
        for number in range(1, 8):
            conductivity = jnp.where(where == number, cond[number], conductivity)
        packed = jnp.zeros((8, BZ), jnp.float32)
        for field in range(6):
            if field < 3:
                value = rhs[field, x]
            else:
                c = field - 3
                value = jnp.where(flags[c, x] == 0, conductivity * fraction[c, x], 0.0)
                sigma[c, x] = value
                first_iter[c, x] = weigh(value) * rhs[c, x]
            for tile in range(2):
                slot = field * 2 + tile
                moved = rotate(value[tile * 8 : tile * 8 + 8], LOW + 8 * slot, 1)
                packed = jnp.where(group == slot, moved, packed)
        packed_out[x] = packed


def send_y(ypar, zpar, rhs, sigma, first_iter, from_even, from_odd, first_out, second_out, packed):
    below = (lanes((8, BZ)) % 8) < LOW
    odd = (lanes((4, BZ)) // 8) % 2
    below = below == (zpar[0] == 0)
    for x in range(BX):
        packed[x] = jnp.where(below, jnp.where(zpar[0] == 0, from_odd[0, x], from_odd[1, x]), from_even[x])

    def fill(out, layout, side):
        for p in OWN:
            for c in range(3):
                (at, count), (at_sigma, both) = layout[p, c], layout[p, c + 3]
                inner = 0 if side == ABOVE else BY - both
                outer = both if side == ABOVE else BY - count
                out[at_sigma : at_sigma + both] = sigma[c, p - LOW, inner : inner + both]
                place = at if side == ABOVE else at + count - both
                out[place : place + both] = rhs[c, p - LOW, inner : inner + both]
                place = at + both if side == ABOVE else at
                out[place : place + count - both] = first_iter[c, p - LOW, outer : outer + count - both]
        start = 0 if side == ABOVE else 4
        for p in OWN[::2]:
            value = packed[p - LOW, start : start + 4]
            other = packed[p + 1 - LOW, start : start + 4]
            at = layout[p, "packed"]
            out[at : at + 4] = jnp.where(odd == 1 - side, value, rotate(other, 8 if side == ABOVE else -8, 1))

    @pl.when(ypar[0] == 0)
    def _():
        fill(first_out, Y_LOW, BELOW)
        fill(second_out, Y_HIGH, ABOVE)

    @pl.when(ypar[0] != 0)
    def _():
        fill(second_out, Y_LOW, BELOW)
        fill(first_out, Y_HIGH, ABOVE)


def own_edge(p, y_low, y_high):
    odd = (lanes((4, BZ)) // 8) % 2 == 1
    above = y_high[Y_HIGH[p, "packed"] : Y_HIGH[p, "packed"] + 4]
    below = y_low[Y_LOW[p, "packed"] : Y_LOW[p, "packed"] + 4]
    if (p - LOW) % 2:
        above, below = rotate(above, -8, 1), rotate(below, 8, 1)
    return jnp.where(odd, below, above)


def first_lanes(p, value):
    fields = [c for c in range(3) if plane_need(c, p) == 1]
    if not fields:
        return value
    field = lanes(value.shape) // 16
    chosen = (field >= fields[0]) & (field <= fields[-1])
    return jnp.where(chosen, weigh(rotate(value, -48, 1)) * value, value)


def send_x(ypar, rhs, sigma, first_iter, packed, first, second, up_out, down_out, y_low, y_high):
    even = ypar[0] == 0
    y_high[...] = jnp.where(even, first[1], second[1])
    y_low[...] = jnp.where(even, second[0], first[0])
    for out, layout, planes, step in (
        (up_out, X_LOW, range(LOW), BX),
        (down_out, X_HIGH, range(LOW + BX, EXT), -BX),
    ):
        for p in planes:
            own = p + step
            x = own - LOW
            at = layout[p, "packed"]
            out[at : at + 8] = first_lanes(p, packed[x])
            at = layout[p, "edge"]
            out[at : at + 4] = first_lanes(p, own_edge(own, y_low, y_high))
            for c in range(3):
                if plane_need(c, p) == 2:
                    at = layout[p, c]
                    out[at : at + BY] = rhs[c, x]
                    at = layout[p, c + 3]
                    out[at : at + BY] = sigma[c, x]
                elif plane_need(c, p) == 1:
                    at = layout[p, c]
                    out[at : at + BY] = first_iter[c, x]
                for side, source, have in ((BELOW, y_low, Y_LOW), (ABOVE, y_high, Y_HIGH)):
                    (at, count), (at_sigma, both) = layout[p, c, side], layout[p, c + 3, side]
                    (own_at, own_count), (own_sigma, own_both) = have[own, c], have[own, c + 3]

                    def rows(base, size, near, far):
                        return slice(base + near, base + far) if side == ABOVE else slice(base + size - far, base + size - near)

                    if both:
                        out[rows(at_sigma, both, 0, both)] = source[rows(own_sigma, own_both, 0, both)]
                        out[rows(at, count, 0, both)] = source[rows(own_at, own_count, 0, both)]
                    middle = min(max(both, own_both), count)
                    if both < middle:
                        out[rows(at, count, both, middle)] = (
                            weigh(source[rows(own_sigma, own_both, both, middle)])
                            * source[rows(own_at, own_count, both, middle)]
                        )
                    if middle < count:
                        out[rows(at, count, middle, count)] = source[rows(own_at, own_count, middle, count)]


def up_y(v):
    return rotate(v, -1, 0)


def down_y(v):
    return rotate(v, 1, 0)


def up_z(v):
    return rotate(v, -1, 1)


def down_z(v):
    return rotate(v, 1, 1)


def spread(p, main, tile, packed, edge, wide, weight, iterate):
    edge = jnp.concatenate([edge, rotate(edge, -8, 1)], axis=0)
    row = lax.broadcasted_iota(jnp.int32, (8, BZ), 0)

    def parts(field):
        at = LOW + 16 * field
        return (
            (slice(0, BY), slice(0, BZ), main(field)),
            (slice(BY, 24), slice(0, BZ), tile(field)),
            (slice(0, 8), slice(BZ, None), rotate(packed, -at, 1)),
            (slice(8, BY), slice(BZ, None), rotate(packed, -(at + 8), 1)),
            (slice(BY, 24), slice(BZ, None), rotate(edge, -at, 1)),
        )

    for c in range(3):
        need = plane_need(c, p)
        if need == 0:
            continue
        if need == 1:
            for rows, columns, value in parts(c):
                iterate(c, p)[rows, columns] = value
            continue
        (low_any, low_both), (high_any, high_both) = row_counts(c, p)
        single = ((row >= high_both) & (row < high_any)) | ((row >= 8 - low_any) & (row < 8 - low_both))
        for i, ((rows, columns, rhs), (_, _, sigma)) in enumerate(zip(parts(c), parts(3 + c))):
            w = weigh(sigma)
            u = w * rhs
            if i == 1 and (high_any > high_both or low_any > low_both):
                u = jnp.where(single, rhs, u)
            wide(c, p)[rows, columns] = rhs
            wide(3 + c, p)[rows, columns] = sigma
            weight(c, p)[rows, columns] = w
            iterate(c, p)[rows, columns] = u


def faces(u, p):
    u0, u1, u2 = u(0, p)[...], u(1, p)[...], u(2, p)[...]
    f0 = (up_y(u2) - u2) - (up_z(u1) - u1)
    f1 = (up_z(u0) - u0) - (u(2, p + 1)[...] - u2)
    f2 = (u(1, p + 1)[...] - u1) - (up_y(u0) - u0)
    return f0, f1, f2


def curl0(f):
    return (down_z(f[1]) - f[1]) - (down_y(f[2]) - f[2])


def curl1(f, prev):
    return (prev[2] - f[2]) - (down_z(f[0]) - f[0])


def curl2(f, prev):
    return (down_y(f[0]) - f[0]) - (prev[1] - f[1])


def update(c, p, k, wide, weight, iterate):
    u = iterate(c, p)[...]
    return u + weight(c, p)[...] * (wide(c, p)[...] - (k + wide(3 + c, p)[...] * u))


def smooth(planes, prev, wide, weight, iterate, second_iter):
    for p in planes:
        f = faces(iterate, p)
        for c, k in enumerate((curl0(f), curl1(f, prev), curl2(f, prev))):
            second_iter(c, p)[...] = update(c, p, k, wide, weight, iterate)
        prev = f
    return prev


def defect(c, p, k, wide, second_iter):
    return wide(c, p)[...] - (k + wide(3 + c, p)[...] * second_iter(c, p)[...])


def kept(c, p, value, wide):
    return jnp.where(wide(3 + c, p)[...] > 0.0, value, 0.0)


def gather_nodes(p, before, q0, q1, q2, nodal):
    d1, d2 = down_y(q1), down_z(q2)
    nodal(0, p)[...] = (before - q0) + (d1 - q1) + (d2 - q2)
    nodal(1, p)[...] = (before + q0) * 0.5
    nodal(2, p)[...] = (d1 + q1) * 0.5
    nodal(3, p)[...] = (d2 + q2) * 0.5


def restrict(planes, prev, before, wide, second_iter, nodal):
    for p in planes:
        f = faces(second_iter, p)
        q = [
            kept(c, p, defect(c, p, k, wide, second_iter), wide)
            for c, k in enumerate((curl0(f), curl1(f, prev), curl2(f, prev)))
        ]
        gather_nodes(p, before, *q, nodal)
        prev, before = f, q[0]
    return prev, before


def beside(c, p, nodal):
    b = nodal(c, p)[...]
    return (1.2 * NODE) * b + (NODE * NODE) * ((up_y(b) + down_y(b)) + (up_z(b) + down_z(b)))


def finish(p, n0, n0_next, n1, n1_next, n2, n3, second_iter, rhs, sigma):
    corrections = (
        (n0_next - n0) + (n1_next + n1) * 0.5,
        (up_y(n0) - n0) + (n2 + up_y(n2)) * 0.5,
        (up_z(n0) - n0) + (n3 + up_z(n3)) * 0.5,
    )
    return [
        jnp.where(
            sigma[c, p - LOW] > 0.0,
            second_iter(c, p)[0:BY, 0:BZ] + corrections[c][0:BY, 0:BZ],
            0.96 * rhs[c, p - LOW],
        )
        for c in range(3)
    ]


INNER = {"wide": OWN, "weight": OWN, "iterate": OWN, "second": OWN[1:-1], "nodal": OWN[2:-2]}
USED = {"wide": range(EXT), "weight": range(EXT), "iterate": range(EXT), "second": range(1, EXT - 1), "nodal": range(2, EXT - 2)}
OUTER = {name: [p for p in USED[name] if p not in INNER[name]] for name in USED}
INNER |= {"second_part": OWN[:1], "second_carry": OWN[-2:-1], "nodal_part": OWN[1:2], "nodal_carry": OWN[-3:-2], "beside": OWN[2:-2]}
FIELDS = {
    "wide": 6, "weight": 3, "iterate": 3, "second": 3, "nodal": 4,
    "second_part": 3, "second_carry": 2, "nodal_part": 3, "nodal_carry": 3, "beside": 4,
}
MIDDLE = OWN[3]


def plane_arrays(kind, inner, outer=None):
    at = {p: (inner, i) for i, p in enumerate(INNER[kind])}
    if outer is not None:
        at.update({p: (outer, i) for i, p in enumerate(OUTER[kind])})
    return lambda c, p: at[p][0].at[c, at[p][1]]


def stencil_inner(rhs, sigma, packed, y_low, y_high, middle, *arrays):
    wide, weight, iterate, second_iter, nodal, second_part, second_carry, nodal_part, nodal_carry, near = (
        plane_arrays(kind, ref) for kind, ref in zip(FIELDS, arrays)
    )
    for p in OWN:

        def main(field):
            return (rhs if field < 3 else sigma)[field % 3, p - LOW]

        def tile(field):
            target = wide(field, p)
            for ref, layout, below in ((y_low, Y_LOW, True), (y_high, Y_HIGH, False)):
                at, count = layout[p, field]
                start = 24 - count if below else BY
                target[start : start + count, 0:BZ] = ref[at : at + count]
            return target[BY:24, 0:BZ]

        spread(p, main, tile, packed[p - LOW], own_edge(p, y_low, y_high), wide, weight, iterate)

    p = OWN[0]
    prev = f = faces(iterate, p)
    k = (curl0(f), -f[2] - (down_z(f[0]) - f[0]), (down_y(f[0]) - f[0]) + f[1])
    for c in range(3):
        second_part(c, p)[...] = update(c, p, k[c], wide, weight, iterate)
    prev = smooth(INNER["second"], prev, wide, weight, iterate, second_iter)
    for i in range(2):
        second_carry(i, INNER["second"][-1])[...] = prev[1 + i]

    p = OWN[1]
    prev = f = faces(second_iter, p)
    before = kept(0, p, defect(0, p, curl0(f), wide, second_iter), wide)
    nodal_part(0, p)[...] = before
    nodal_part(1, p)[...] = defect(1, p, -f[2] - (down_z(f[0]) - f[0]), wide, second_iter)
    nodal_part(2, p)[...] = defect(2, p, (down_y(f[0]) - f[0]) + f[1], wide, second_iter)
    prev, before = restrict(INNER["nodal"], prev, before, wide, second_iter, nodal)
    for i, value in enumerate((prev[1], prev[2], before)):
        nodal_carry(i, INNER["nodal"][-1])[...] = value

    for p in INNER["beside"]:
        for c in range(4):
            near(c, p)[...] = beside(c, p, nodal)

    def node(c, p):
        return near(c, p)[...] + (NODE * NODE) * (nodal(c, p - 1)[...] + nodal(c, p + 1)[...])

    p = MIDDLE
    planes = finish(
        p, node(0, p), node(0, p + 1), node(1, p), node(1, p + 1), node(2, p), node(3, p), second_iter, rhs, sigma
    )
    for c in range(3):
        middle[c] = planes[c]


def stencil_outer(rhs, sigma, low, high, middle, *arrays):
    inner, out, outer = arrays[: len(FIELDS)], arrays[len(FIELDS)], arrays[len(FIELDS) + 1 :]
    wide, weight, iterate, second_iter, nodal = (plane_arrays(k, *refs) for k, refs in zip(FIELDS, zip(inner, outer)))
    second_part, second_carry, nodal_part, nodal_carry, near = (
        plane_arrays(kind, ref) for kind, ref in list(zip(FIELDS, inner))[5:]
    )
    upper = lax.broadcasted_iota(jnp.int32, (8, BZ), 0) < 4
    for p in OUTER["wide"]:
        ref, layout = (low, X_LOW) if p < LOW else (high, X_HIGH)

        def main(field):
            return ref[layout[p, field] : layout[p, field] + BY]

        def tile(field):
            (below, count), (above, _) = layout[p, field, BELOW], layout[p, field, ABOVE]
            return jnp.where(upper, ref[above : above + 8], ref[below + count - 8 : below + count])

        packed, edge = layout[p, "packed"], layout[p, "edge"]
        spread(p, main, tile, ref[packed : packed + 8], ref[edge : edge + 4], wide, weight, iterate)

    first, last = INNER["second"][0] - 1, INNER["second"][-1]
    prev = smooth(range(1, first), faces(iterate, 0), wide, weight, iterate, second_iter)
    second_iter(0, first)[...] = second_part(0, first)[...]
    second_iter(1, first)[...] = second_part(1, first)[...] - weight(1, first)[...] * prev[2]
    second_iter(2, first)[...] = second_part(2, first)[...] + weight(2, first)[...] * prev[1]
    prev = (None, second_carry(0, last)[...], second_carry(1, last)[...])
    smooth(range(last + 1, EXT - 1), prev, wide, weight, iterate, second_iter)

    first, last = INNER["nodal"][0] - 1, INNER["nodal"][-1]
    prev = faces(second_iter, 1)
    before = kept(0, 1, defect(0, 1, curl0(prev), wide, second_iter), wide)
    prev, before = restrict(range(2, first), prev, before, wide, second_iter, nodal)
    q1 = kept(1, first, nodal_part(1, first)[...] - prev[2], wide)
    q2 = kept(2, first, nodal_part(2, first)[...] + prev[1], wide)
    gather_nodes(first, before, nodal_part(0, first)[...], q1, q2, nodal)
    prev = (None, nodal_carry(0, last)[...], nodal_carry(1, last)[...])
    restrict(range(last + 1, EXT - 2), prev, nodal_carry(2, last)[...], wide, second_iter, nodal)

    def node(c, p):
        own = near(c, p)[...] if p in INNER["beside"] else beside(c, p, nodal)
        return own + (NODE * NODE) * (nodal(c, p - 1)[...] + nodal(c, p + 1)[...])

    n0, n1 = node(0, LOW), node(1, LOW)
    for p in OWN:
        n0_next, n1_next = node(0, p + 1), node(1, p + 1)
        if p == MIDDLE:
            planes = [middle[c] for c in range(3)]
        else:
            planes = finish(p, n0, n0_next, n1, n1_next, node(2, p), node(3, p), second_iter, rhs, sigma)
        for c in range(3):
            out[c, p - LOW] = planes[c]
        n0, n1 = n0_next, n1_next


def pairs(count):
    return (
        [[i, i + 1] for i in range(0, count, 2)],
        [[i, (i + 1) % count] for i in range(1, count, 2)],
    )


def gather(value, axis, groups):
    return lax.all_gather(value, axis, axis=0, tiled=False, axis_index_groups=groups)


def shift(value, axis, step):
    count = lax.axis_size(axis)
    return lax.ppermute(value, axis, [(i, (i + step) % count) for i in range(count)])


def on_device(rhs, conductivity, fraction, region, flags):
    f32 = functools.partial(jax.ShapeDtypeStruct, dtype=jnp.float32)
    ypar = (lax.axis_index("gy") & 1).astype(jnp.int32).reshape(1)
    zpar = (lax.rem(lax.axis_index("gz"), 2)).astype(jnp.int32).reshape(1)

    block = f32((3, BX, BY, BZ))
    lane_block = f32((BX, 8, BZ))
    rhs, sigma, first_iter, packed = call(
        prepare,
        (block, block, block, lane_block),
        [HBM] * 5,
        scratch=(
            pltpu.SMEM((8,), jnp.float32),
            pltpu.VMEM((3, BX, BY, BZ), jnp.float32),
            pltpu.VMEM((BX, BY, BZ), jnp.int32),
            pltpu.VMEM((3, BX, BY, BZ), jnp.int32),
            pltpu.SemaphoreType.DMA((5,)),
        ),
    )(*(pltpu.with_memory_space_constraint(a, pltpu.HBM) for a in (conductivity, rhs, fraction, region, flags)))

    from_even = lax.ppermute(packed, "gz", [(i, i ^ 1) for i in range(lax.axis_size("gz"))])
    from_odd = gather(packed, "gz", pairs(lax.axis_size("gz"))[1])

    even_y, odd_y = pairs(lax.axis_size("gy"))
    payload = f32((Y_ROWS, BZ))
    to_first, to_second, packed = call(
        send_y, (payload, payload, lane_block), [SMEM] * 2 + [VMEM] * 5
    )(ypar, zpar, rhs, sigma, first_iter, from_even, from_odd)
    first = gather(to_first, "gy", even_y)
    second = gather(to_second, "gy", odd_y)

    up, down, y_low, y_high = call(
        send_x, (f32((X_LOW_ROWS, BZ)), f32((X_HIGH_ROWS, BZ)), payload, payload), [SMEM] + [VMEM] * 6
    )(ypar, rhs, sigma, first_iter, packed, first, second)
    low = shift(up, "gx", 1)
    high = shift(down, "gx", -1)

    inner = call(
        stencil_inner,
        (f32((3, BY, BZ)), *(f32((FIELDS[kind], len(INNER[kind]), 24, 2 * BZ)) for kind in FIELDS)),
        [VMEM] * 5,
        flops=20000000,
    )(rhs, sigma, packed, y_low, y_high)
    return call(
        stencil_outer,
        block,
        [VMEM] * (5 + len(FIELDS)),
        scratch=[pltpu.VMEM((FIELDS[kind], len(OUTER[kind]), 24, 2 * BZ), jnp.float32) for kind in OUTER],
    )(rhs, sigma, low, high, *inner)


def solution(mesh):
    return jax.shard_map(
        on_device,
        mesh=mesh,
        in_specs=(
            P(None, "gx", "gy", "gz"),
            P(),
            P(None, "gx", "gy", "gz"),
            P("gx", "gy", "gz"),
            P(None, "gx", "gy", "gz"),
        ),
        out_specs=P(None, "gx", "gy", "gz"),
        check_vma=False,
    )
```

```python
import functools

import jax
import jax.numpy as jnp
import numpy as np
from jax import lax
from jax.experimental import pallas as pl
from jax.experimental.pallas import tpu as pltpu
from jax.sharding import PartitionSpec as P


EDGE = 0.8
NODE = 0.8 / 7.0

BX, BY, BZ = 8, 16, 128
LOW, HIGH = 3, 4
EXT = LOW + BX + HIGH
VMEM_LIMIT = 16 * 1024 * 1024

VMEM = pl.BlockSpec(memory_space=pltpu.VMEM)
SMEM = pl.BlockSpec(memory_space=pltpu.SMEM)
HBM = pl.BlockSpec(memory_space=pltpu.HBM)


def halo_need():
    size = BX + 9

    def at(need, axis, k):
        return np.roll(need, k, axis)

    out = np.zeros((3, size, size, size), bool)
    out[:, 4 : 4 + BX, 4 : 4 + BX, 4 : 4 + BX] = True
    node = np.zeros((4, size, size, size), bool)
    for a in range(3):
        both = out[a] | at(out[a], a, 1)
        node[0] |= both
        node[a + 1] |= both
    near = node.copy()
    for a in range(3):
        near |= np.roll(node, 1, a + 1) | np.roll(node, -1, a + 1)
    masked = np.stack([near[0] | at(near[0], a, -1) | near[a + 1] | at(near[a + 1], a, -1) for a in range(3)])

    def operand(need):
        face = np.zeros_like(need)
        for a in range(3):
            b, c = (a + 1) % 3, (a + 2) % 3
            face[b] |= need[a] | at(need[a], c, -1)
            face[c] |= need[a] | at(need[a], b, -1)
        edge = need.copy()
        for a in range(3):
            b, c = (a + 1) % 3, (a + 2) % 3
            edge[b] |= face[a] | at(face[a], c, 1)
            edge[c] |= face[a] | at(face[a], b, 1)
        return edge

    second = operand(masked) | out
    first = operand(second)
    return second.any(3).astype(int) + first.any(3).astype(int)


NEED = halo_need()


def plane_need(c, p):
    return NEED[c, p - LOW + 4].max()


def row_counts(c, p):
    need = NEED[c, p - LOW + 4]
    below, above = need[:4], need[4 + BX :]
    return tuple((int((side > 0).sum()), int((side > 1).sum())) for side in (below, above))


OWN = range(LOW, LOW + BX)
BELOW, ABOVE = 0, 1


def y_layout(side):
    at, rows = {}, 0
    for p in OWN:
        for field in range(6):
            count = row_counts(field % 3, p)[side][field // 3]
            at[p, field] = (rows, count)
            rows += count
    rows = -(-rows // 8) * 8
    for p in OWN[::2]:
        at[p, "packed"] = at[p + 1, "packed"] = rows
        rows += 4
    return at, rows


Y_LOW, Y_LOW_ROWS = y_layout(BELOW)
Y_HIGH, Y_HIGH_ROWS = y_layout(ABOVE)
Y_ROWS = -(-max(Y_LOW_ROWS, Y_HIGH_ROWS) // 8) * 8


def x_layout(planes):
    at, rows = {}, 0
    for p in planes:
        for field in range(6):
            if plane_need(field % 3, p) > field // 3:
                at[p, field] = rows
                rows += BY
    for p in planes:
        for field in range(6):
            for side in (BELOW, ABOVE):
                count = row_counts(field % 3, p)[side][field // 3]
                at[p, field, side] = (rows, count)
                rows += count
    rows = -(-rows // 4) * 4
    for p in planes:
        at[p, "edge"] = rows
        rows += 4
    rows = -(-rows // 8) * 8
    for p in planes:
        at[p, "packed"] = rows
        rows += 8
    return at, -(-rows // 8) * 8


X_LOW, X_LOW_ROWS = x_layout(range(LOW))
X_HIGH, X_HIGH_ROWS = x_layout(range(LOW + BX, EXT))


def call(body, out_shape, specs, scratch=(), flops=1000000):
    return pl.pallas_call(
        body,
        out_shape=out_shape,
        in_specs=specs,
        out_specs=jax.tree.map(lambda _: VMEM, out_shape),
        scratch_shapes=list(scratch),
        compiler_params=pltpu.CompilerParams(vmem_limit_bytes=VMEM_LIMIT),
        cost_estimate=pl.CostEstimate(flops=flops, bytes_accessed=1000000, transcendentals=0),
    )


def lanes(shape):
    return lax.broadcasted_iota(jnp.int32, shape, 1)


def rotate(v, shift, axis):
    return pltpu.roll(v, shift % v.shape[axis], axis)


def weigh(sigma):
    return jnp.where(sigma > 0.0, EDGE / (4.0 + sigma), 0.0)


def prepare(cond_in, rhs_in, fraction_in, region_in, flags_in, rhs, sigma, first_iter, packed_out, cond, fraction, region, flags, sems):
    copies = [
        pltpu.make_async_copy(source, target, sems.at[i])
        for i, (source, target) in enumerate(
            ((cond_in, cond), (region_in, region), (fraction_in, fraction), (flags_in, flags), (rhs_in, rhs))
        )
    ]
    for copy in copies:
        copy.start()
    for copy in copies:
        copy.wait()
    group = lanes((8, BZ)) // 8
    for x in range(BX):
        where = region[x]
        conductivity = jnp.full((BY, BZ), cond[0], jnp.float32)
        for number in range(1, 8):
            conductivity = jnp.where(where == number, cond[number], conductivity)
        packed = jnp.zeros((8, BZ), jnp.float32)
        for field in range(6):
            if field < 3:
                value = rhs[field, x]
            else:
                c = field - 3
                value = jnp.where(flags[c, x] == 0, conductivity * fraction[c, x], 0.0)
                sigma[c, x] = value
                first_iter[c, x] = weigh(value) * rhs[c, x]
            for tile in range(2):
                slot = field * 2 + tile
                moved = rotate(value[tile * 8 : tile * 8 + 8], LOW + 8 * slot, 1)
                packed = jnp.where(group == slot, moved, packed)
        packed_out[x] = packed


def send_y(
    ypar, zpar, zlast, rhs, sigma, first_iter, from_even, from_odd, from_last, first_out, second_out, packed
):
    below = (lanes((8, BZ)) % 8) < LOW
    odd = (lanes((4, BZ)) // 8) % 2
    below = below == (zpar[0] == 0)
    for x in range(BX):
        packed[x] = jnp.where(below, jnp.where(zpar[0] == 0, from_odd[0, x], from_odd[1, x]), jnp.where(zlast[0] == 0, from_even[x], from_last[x]))

    def fill(out, layout, side):
        for p in OWN:
            for c in range(3):
                (at, count), (at_sigma, both) = layout[p, c], layout[p, c + 3]
                inner = 0 if side == ABOVE else BY - both
                outer = both if side == ABOVE else BY - count
                out[at_sigma : at_sigma + both] = sigma[c, p - LOW, inner : inner + both]
                place = at if side == ABOVE else at + count - both
                out[place : place + both] = rhs[c, p - LOW, inner : inner + both]
                place = at + both if side == ABOVE else at
                out[place : place + count - both] = first_iter[c, p - LOW, outer : outer + count - both]
        start = 0 if side == ABOVE else 4
        for p in OWN[::2]:
            value = packed[p - LOW, start : start + 4]
            other = packed[p + 1 - LOW, start : start + 4]
            at = layout[p, "packed"]
            out[at : at + 4] = jnp.where(odd == 1 - side, value, rotate(other, 8 if side == ABOVE else -8, 1))

    @pl.when(ypar[0] == 0)
    def _():
        fill(first_out, Y_LOW, BELOW)
        fill(second_out, Y_HIGH, ABOVE)

    @pl.when(ypar[0] != 0)
    def _():
        fill(second_out, Y_LOW, BELOW)
        fill(first_out, Y_HIGH, ABOVE)


def own_edge(p, y_low, y_high):
    odd = (lanes((4, BZ)) // 8) % 2 == 1
    above = y_high[Y_HIGH[p, "packed"] : Y_HIGH[p, "packed"] + 4]
    below = y_low[Y_LOW[p, "packed"] : Y_LOW[p, "packed"] + 4]
    if (p - LOW) % 2:
        above, below = rotate(above, -8, 1), rotate(below, 8, 1)
    return jnp.where(odd, below, above)


def first_lanes(p, value):
    fields = [c for c in range(3) if plane_need(c, p) == 1]
    if not fields:
        return value
    field = lanes(value.shape) // 16
    chosen = (field >= fields[0]) & (field <= fields[-1])
    return jnp.where(chosen, weigh(rotate(value, -48, 1)) * value, value)


def send_x(ypar, rhs, sigma, first_iter, packed, first, second, up_out, down_out, y_low, y_high):
    even = ypar[0] == 0
    y_high[...] = jnp.where(even, first[1], second[1])
    y_low[...] = jnp.where(even, second[0], first[0])
    for out, layout, planes, step in (
        (up_out, X_LOW, range(LOW), BX),
        (down_out, X_HIGH, range(LOW + BX, EXT), -BX),
    ):
        for p in planes:
            own = p + step
            x = own - LOW
            at = layout[p, "packed"]
            out[at : at + 8] = first_lanes(p, packed[x])
            at = layout[p, "edge"]
            out[at : at + 4] = first_lanes(p, own_edge(own, y_low, y_high))
            for c in range(3):
                if plane_need(c, p) == 2:
                    at = layout[p, c]
                    out[at : at + BY] = rhs[c, x]
                    at = layout[p, c + 3]
                    out[at : at + BY] = sigma[c, x]
                elif plane_need(c, p) == 1:
                    at = layout[p, c]
                    out[at : at + BY] = first_iter[c, x]
                for side, source, have in ((BELOW, y_low, Y_LOW), (ABOVE, y_high, Y_HIGH)):
                    (at, count), (at_sigma, both) = layout[p, c, side], layout[p, c + 3, side]
                    (own_at, own_count), (own_sigma, own_both) = have[own, c], have[own, c + 3]

                    def rows(base, size, near, far):
                        return slice(base + near, base + far) if side == ABOVE else slice(base + size - far, base + size - near)

                    if both:
                        out[rows(at_sigma, both, 0, both)] = source[rows(own_sigma, own_both, 0, both)]
                        out[rows(at, count, 0, both)] = source[rows(own_at, own_count, 0, both)]
                    middle = min(max(both, own_both), count)
                    if both < middle:
                        out[rows(at, count, both, middle)] = (
                            weigh(source[rows(own_sigma, own_both, both, middle)])
                            * source[rows(own_at, own_count, both, middle)]
                        )
                    if middle < count:
                        out[rows(at, count, middle, count)] = source[rows(own_at, own_count, middle, count)]


def up_y(v):
    return rotate(v, -1, 0)


def down_y(v):
    return rotate(v, 1, 0)


def up_z(v):
    return rotate(v, -1, 1)


def down_z(v):
    return rotate(v, 1, 1)


def spread(p, main, tile, packed, edge, wide, weight, iterate):
    edge = jnp.concatenate([edge, rotate(edge, -8, 1)], axis=0)
    row = lax.broadcasted_iota(jnp.int32, (8, BZ), 0)

    def parts(field):
        at = LOW + 16 * field
        return (
            (slice(0, BY), slice(0, BZ), main(field)),
            (slice(BY, 24), slice(0, BZ), tile(field)),
            (slice(0, 8), slice(BZ, None), rotate(packed, -at, 1)),
            (slice(8, BY), slice(BZ, None), rotate(packed, -(at + 8), 1)),
            (slice(BY, 24), slice(BZ, None), rotate(edge, -at, 1)),
        )

    for c in range(3):
        need = plane_need(c, p)
        if need == 0:
            continue
        if need == 1:
            for rows, columns, value in parts(c):
                iterate(c, p)[rows, columns] = value
            continue
        (low_any, low_both), (high_any, high_both) = row_counts(c, p)
        single = ((row >= high_both) & (row < high_any)) | ((row >= 8 - low_any) & (row < 8 - low_both))
        for i, ((rows, columns, rhs), (_, _, sigma)) in enumerate(zip(parts(c), parts(3 + c))):
            w = weigh(sigma)
            u = w * rhs
            if i == 1 and (high_any > high_both or low_any > low_both):
                u = jnp.where(single, rhs, u)
            wide(c, p)[rows, columns] = rhs
            wide(3 + c, p)[rows, columns] = sigma
            weight(c, p)[rows, columns] = w
            iterate(c, p)[rows, columns] = u


def faces(u, p):
    u0, u1, u2 = u(0, p)[...], u(1, p)[...], u(2, p)[...]
    f0 = (up_y(u2) - u2) - (up_z(u1) - u1)
    f1 = (up_z(u0) - u0) - (u(2, p + 1)[...] - u2)
    f2 = (u(1, p + 1)[...] - u1) - (up_y(u0) - u0)
    return f0, f1, f2


def curl0(f):
    return (down_z(f[1]) - f[1]) - (down_y(f[2]) - f[2])


def curl1(f, prev):
    return (prev[2] - f[2]) - (down_z(f[0]) - f[0])


def curl2(f, prev):
    return (down_y(f[0]) - f[0]) - (prev[1] - f[1])


def update(c, p, k, wide, weight, iterate):
    u = iterate(c, p)[...]
    return u + weight(c, p)[...] * (wide(c, p)[...] - (k + wide(3 + c, p)[...] * u))


def smooth(planes, prev, wide, weight, iterate, second_iter):
    for p in planes:
        f = faces(iterate, p)
        for c, k in enumerate((curl0(f), curl1(f, prev), curl2(f, prev))):
            second_iter(c, p)[...] = update(c, p, k, wide, weight, iterate)
        prev = f
    return prev


def defect(c, p, k, wide, second_iter):
    return wide(c, p)[...] - (k + wide(3 + c, p)[...] * second_iter(c, p)[...])


def kept(c, p, value, wide):
    return jnp.where(wide(3 + c, p)[...] > 0.0, value, 0.0)


def gather_nodes(p, before, q0, q1, q2, nodal):
    d1, d2 = down_y(q1), down_z(q2)
    nodal(0, p)[...] = (before - q0) + (d1 - q1) + (d2 - q2)
    nodal(1, p)[...] = (before + q0) * 0.5
    nodal(2, p)[...] = (d1 + q1) * 0.5
    nodal(3, p)[...] = (d2 + q2) * 0.5


def restrict(planes, prev, before, wide, second_iter, nodal):
    for p in planes:
        f = faces(second_iter, p)
        q = [
            kept(c, p, defect(c, p, k, wide, second_iter), wide)
            for c, k in enumerate((curl0(f), curl1(f, prev), curl2(f, prev)))
        ]
        gather_nodes(p, before, *q, nodal)
        prev, before = f, q[0]
    return prev, before


def beside(c, p, nodal):
    b = nodal(c, p)[...]
    return (1.2 * NODE) * b + (NODE * NODE) * ((up_y(b) + down_y(b)) + (up_z(b) + down_z(b)))


def finish(p, n0, n0_next, n1, n1_next, n2, n3, second_iter, rhs, sigma):
    corrections = (
        (n0_next - n0) + (n1_next + n1) * 0.5,
        (up_y(n0) - n0) + (n2 + up_y(n2)) * 0.5,
        (up_z(n0) - n0) + (n3 + up_z(n3)) * 0.5,
    )
    return [
        jnp.where(
            sigma[c, p - LOW] > 0.0,
            second_iter(c, p)[0:BY, 0:BZ] + corrections[c][0:BY, 0:BZ],
            0.96 * rhs[c, p - LOW],
        )
        for c in range(3)
    ]


INNER = {"wide": OWN, "weight": OWN, "iterate": OWN, "second": OWN[1:-1], "nodal": OWN[2:-2]}
USED = {"wide": range(EXT), "weight": range(EXT), "iterate": range(EXT), "second": range(1, EXT - 1), "nodal": range(2, EXT - 2)}
OUTER = {name: [p for p in USED[name] if p not in INNER[name]] for name in USED}
INNER |= {"second_part": OWN[:1], "second_carry": OWN[-2:-1], "nodal_part": OWN[1:2], "nodal_carry": OWN[-3:-2], "beside": OWN[2:-2]}
FIELDS = {
    "wide": 6, "weight": 3, "iterate": 3, "second": 3, "nodal": 4,
    "second_part": 3, "second_carry": 2, "nodal_part": 3, "nodal_carry": 3, "beside": 4,
}
MIDDLE = OWN[3]


def plane_arrays(kind, inner, outer=None):
    at = {p: (inner, i) for i, p in enumerate(INNER[kind])}
    if outer is not None:
        at.update({p: (outer, i) for i, p in enumerate(OUTER[kind])})
    return lambda c, p: at[p][0].at[c, at[p][1]]


def stencil_inner(rhs, sigma, packed, y_low, y_high, middle, *arrays):
    wide, weight, iterate, second_iter, nodal, second_part, second_carry, nodal_part, nodal_carry, near = (
        plane_arrays(kind, ref) for kind, ref in zip(FIELDS, arrays)
    )
    for p in OWN:

        def main(field):
            return (rhs if field < 3 else sigma)[field % 3, p - LOW]

        def tile(field):
            target = wide(field, p)
            for ref, layout, below in ((y_low, Y_LOW, True), (y_high, Y_HIGH, False)):
                at, count = layout[p, field]
                start = 24 - count if below else BY
                target[start : start + count, 0:BZ] = ref[at : at + count]
            return target[BY:24, 0:BZ]

        spread(p, main, tile, packed[p - LOW], own_edge(p, y_low, y_high), wide, weight, iterate)

    p = OWN[0]
    prev = f = faces(iterate, p)
    k = (curl0(f), -f[2] - (down_z(f[0]) - f[0]), (down_y(f[0]) - f[0]) + f[1])
    for c in range(3):
        second_part(c, p)[...] = update(c, p, k[c], wide, weight, iterate)
    prev = smooth(INNER["second"], prev, wide, weight, iterate, second_iter)
    for i in range(2):
        second_carry(i, INNER["second"][-1])[...] = prev[1 + i]

    p = OWN[1]
    prev = f = faces(second_iter, p)
    before = kept(0, p, defect(0, p, curl0(f), wide, second_iter), wide)
    nodal_part(0, p)[...] = before
    nodal_part(1, p)[...] = defect(1, p, -f[2] - (down_z(f[0]) - f[0]), wide, second_iter)
    nodal_part(2, p)[...] = defect(2, p, (down_y(f[0]) - f[0]) + f[1], wide, second_iter)
    prev, before = restrict(INNER["nodal"], prev, before, wide, second_iter, nodal)
    for i, value in enumerate((prev[1], prev[2], before)):
        nodal_carry(i, INNER["nodal"][-1])[...] = value

    for p in INNER["beside"]:
        for c in range(4):
            near(c, p)[...] = beside(c, p, nodal)

    def node(c, p):
        return near(c, p)[...] + (NODE * NODE) * (nodal(c, p - 1)[...] + nodal(c, p + 1)[...])

    p = MIDDLE
    planes = finish(
        p, node(0, p), node(0, p + 1), node(1, p), node(1, p + 1), node(2, p), node(3, p), second_iter, rhs, sigma
    )
    for c in range(3):
        middle[c] = planes[c]


def stencil_outer(rhs, sigma, low, high, middle, *arrays):
    inner, out, outer = arrays[: len(FIELDS)], arrays[len(FIELDS)], arrays[len(FIELDS) + 1 :]
    wide, weight, iterate, second_iter, nodal = (plane_arrays(k, *refs) for k, refs in zip(FIELDS, zip(inner, outer)))
    second_part, second_carry, nodal_part, nodal_carry, near = (
        plane_arrays(kind, ref) for kind, ref in list(zip(FIELDS, inner))[5:]
    )
    upper = lax.broadcasted_iota(jnp.int32, (8, BZ), 0) < 4
    for p in OUTER["wide"]:
        ref, layout = (low, X_LOW) if p < LOW else (high, X_HIGH)

        def main(field):
            return ref[layout[p, field] : layout[p, field] + BY]

        def tile(field):
            (below, count), (above, _) = layout[p, field, BELOW], layout[p, field, ABOVE]
            return jnp.where(upper, ref[above : above + 8], ref[below + count - 8 : below + count])

        packed, edge = layout[p, "packed"], layout[p, "edge"]
        spread(p, main, tile, ref[packed : packed + 8], ref[edge : edge + 4], wide, weight, iterate)

    first, last = INNER["second"][0] - 1, INNER["second"][-1]
    prev = smooth(range(1, first), faces(iterate, 0), wide, weight, iterate, second_iter)
    second_iter(0, first)[...] = second_part(0, first)[...]
    second_iter(1, first)[...] = second_part(1, first)[...] - weight(1, first)[...] * prev[2]
    second_iter(2, first)[...] = second_part(2, first)[...] + weight(2, first)[...] * prev[1]
    prev = (None, second_carry(0, last)[...], second_carry(1, last)[...])
    smooth(range(last + 1, EXT - 1), prev, wide, weight, iterate, second_iter)

    first, last = INNER["nodal"][0] - 1, INNER["nodal"][-1]
    prev = faces(second_iter, 1)
    before = kept(0, 1, defect(0, 1, curl0(prev), wide, second_iter), wide)
    prev, before = restrict(range(2, first), prev, before, wide, second_iter, nodal)
    q1 = kept(1, first, nodal_part(1, first)[...] - prev[2], wide)
    q2 = kept(2, first, nodal_part(2, first)[...] + prev[1], wide)
    gather_nodes(first, before, nodal_part(0, first)[...], q1, q2, nodal)
    prev = (None, nodal_carry(0, last)[...], nodal_carry(1, last)[...])
    restrict(range(last + 1, EXT - 2), prev, nodal_carry(2, last)[...], wide, second_iter, nodal)

    def node(c, p):
        own = near(c, p)[...] if p in INNER["beside"] else beside(c, p, nodal)
        return own + (NODE * NODE) * (nodal(c, p - 1)[...] + nodal(c, p + 1)[...])

    n0, n1 = node(0, LOW), node(1, LOW)
    for p in OWN:
        n0_next, n1_next = node(0, p + 1), node(1, p + 1)
        if p == MIDDLE:
            planes = [middle[c] for c in range(3)]
        else:
            planes = finish(p, n0, n0_next, n1, n1_next, node(2, p), node(3, p), second_iter, rhs, sigma)
        for c in range(3):
            out[c, p - LOW] = planes[c]
        n0, n1 = n0_next, n1_next


def pairs(count):
    return (
        [[i, i + 1] for i in range(0, count, 2)],
        [[i, (i + 1) % count] for i in range(1, count, 2)],
    )


def gather(value, axis, groups):
    return lax.all_gather(value, axis, axis=0, tiled=False, axis_index_groups=groups)


def shift(value, axis, step):
    count = lax.axis_size(axis)
    return lax.ppermute(value, axis, [(i, (i + step) % count) for i in range(count)])


def on_device(rhs, conductivity, fraction, region, flags):
    f32 = functools.partial(jax.ShapeDtypeStruct, dtype=jnp.float32)
    ypar = (lax.axis_index("gy") & 1).astype(jnp.int32).reshape(1)
    zlast = (lax.axis_index("gz") >= lax.axis_size("gz") - 2).astype(jnp.int32).reshape(1)
    zpar = (lax.rem(lax.axis_index("gz"), 2)).astype(jnp.int32).reshape(1)

    block = f32((3, BX, BY, BZ))
    lane_block = f32((BX, 8, BZ))
    rhs, sigma, first_iter, packed = call(
        prepare,
        (block, block, block, lane_block),
        [HBM] * 5,
        scratch=(
            pltpu.SMEM((8,), jnp.float32),
            pltpu.VMEM((3, BX, BY, BZ), jnp.float32),
            pltpu.VMEM((BX, BY, BZ), jnp.int32),
            pltpu.VMEM((3, BX, BY, BZ), jnp.int32),
            pltpu.SemaphoreType.DMA((5,)),
        ),
    )(*(pltpu.with_memory_space_constraint(a, pltpu.HBM) for a in (conductivity, rhs, fraction, region, flags)))

    nz = lax.axis_size("gz")
    from_even = lax.ppermute(packed, "gz", [(i, i ^ 1) for i in range(nz - 2)])
    from_odd = gather(packed, "gz", pairs(nz)[1])
    from_last = lax.ppermute(packed, "gz", [(nz - 2, nz - 1), (nz - 1, nz - 2)])

    even_y, odd_y = pairs(lax.axis_size("gy"))
    payload = f32((Y_ROWS, BZ))
    to_first, to_second, packed = call(
        send_y, (payload, payload, lane_block), [SMEM] * 3 + [VMEM] * 6
    )(ypar, zpar, zlast, rhs, sigma, first_iter, from_even, from_odd, from_last)
    first = gather(to_first, "gy", even_y)
    second = gather(to_second, "gy", odd_y)

    up, down, y_low, y_high = call(
        send_x, (f32((X_LOW_ROWS, BZ)), f32((X_HIGH_ROWS, BZ)), payload, payload), [SMEM] + [VMEM] * 6
    )(ypar, rhs, sigma, first_iter, packed, first, second)
    low = shift(up, "gx", 1)
    high = shift(down, "gx", -1)

    inner = call(
        stencil_inner,
        (f32((3, BY, BZ)), *(f32((FIELDS[kind], len(INNER[kind]), 24, 2 * BZ)) for kind in FIELDS)),
        [VMEM] * 5,
        flops=20000000,
    )(rhs, sigma, packed, y_low, y_high)
    return call(
        stencil_outer,
        block,
        [VMEM] * (5 + len(FIELDS)),
        scratch=[pltpu.VMEM((FIELDS[kind], len(OUTER[kind]), 24, 2 * BZ), jnp.float32) for kind in OUTER],
    )(rhs, sigma, low, high, *inner)


def solution(mesh):
    return jax.shard_map(
        on_device,
        mesh=mesh,
        in_specs=(
            P(None, "gx", "gy", "gz"),
            P(),
            P(None, "gx", "gy", "gz"),
            P("gx", "gy", "gz"),
            P(None, "gx", "gy", "gz"),
        ),
        out_specs=P(None, "gx", "gy", "gz"),
        check_vma=False,
    )
```

```python
import functools

import jax
import jax.numpy as jnp
import numpy as np
from jax import lax
from jax.experimental import pallas as pl
from jax.experimental.pallas import tpu as pltpu
from jax.sharding import PartitionSpec as P


EDGE = 0.8
NODE = 0.8 / 7.0

BX, BY, BZ = 8, 16, 128
LOW, HIGH = 3, 4
EXT = LOW + BX + HIGH
VMEM_LIMIT = 16 * 1024 * 1024

VMEM = pl.BlockSpec(memory_space=pltpu.VMEM)
SMEM = pl.BlockSpec(memory_space=pltpu.SMEM)
HBM = pl.BlockSpec(memory_space=pltpu.HBM)


def halo_need():
    size = BX + 9

    def at(need, axis, k):
        return np.roll(need, k, axis)

    out = np.zeros((3, size, size, size), bool)
    out[:, 4 : 4 + BX, 4 : 4 + BX, 4 : 4 + BX] = True
    node = np.zeros((4, size, size, size), bool)
    for a in range(3):
        both = out[a] | at(out[a], a, 1)
        node[0] |= both
        node[a + 1] |= both
    near = node.copy()
    for a in range(3):
        near |= np.roll(node, 1, a + 1) | np.roll(node, -1, a + 1)
    masked = np.stack([near[0] | at(near[0], a, -1) | near[a + 1] | at(near[a + 1], a, -1) for a in range(3)])

    def operand(need):
        face = np.zeros_like(need)
        for a in range(3):
            b, c = (a + 1) % 3, (a + 2) % 3
            face[b] |= need[a] | at(need[a], c, -1)
            face[c] |= need[a] | at(need[a], b, -1)
        edge = need.copy()
        for a in range(3):
            b, c = (a + 1) % 3, (a + 2) % 3
            edge[b] |= face[a] | at(face[a], c, 1)
            edge[c] |= face[a] | at(face[a], b, 1)
        return edge

    second = operand(masked) | out
    first = operand(second)
    return second.any(3).astype(int) + first.any(3).astype(int)


NEED = halo_need()


def plane_need(c, p):
    return NEED[c, p - LOW + 4].max()


def row_counts(c, p):
    need = NEED[c, p - LOW + 4]
    below, above = need[:4], need[4 + BX :]
    return tuple((int((side > 0).sum()), int((side > 1).sum())) for side in (below, above))


OWN = range(LOW, LOW + BX)
BELOW, ABOVE = 0, 1


def y_layout(side):
    at, rows = {}, 0
    for p in OWN:
        for field in range(6):
            count = row_counts(field % 3, p)[side][field // 3]
            at[p, field] = (rows, count)
            rows += count
    rows = -(-rows // 8) * 8
    for p in OWN[::2]:
        at[p, "packed"] = at[p + 1, "packed"] = rows
        rows += 4
    return at, rows


Y_LOW, Y_LOW_ROWS = y_layout(BELOW)
Y_HIGH, Y_HIGH_ROWS = y_layout(ABOVE)
Y_ROWS = -(-max(Y_LOW_ROWS, Y_HIGH_ROWS) // 8) * 8


def x_layout(planes):
    at, rows = {}, 0
    for p in planes:
        for field in range(6):
            if plane_need(field % 3, p) > field // 3:
                at[p, field] = rows
                rows += BY
    for p in planes:
        for field in range(6):
            for side in (BELOW, ABOVE):
                count = row_counts(field % 3, p)[side][field // 3]
                at[p, field, side] = (rows, count)
                rows += count
    rows = -(-rows // 4) * 4
    for p in planes:
        at[p, "edge"] = rows
        rows += 4
    rows = -(-rows // 8) * 8
    for p in planes:
        at[p, "packed"] = rows
        rows += 8
    return at, -(-rows // 8) * 8


X_LOW, X_LOW_ROWS = x_layout(range(LOW))
X_HIGH, X_HIGH_ROWS = x_layout(range(LOW + BX, EXT))


def call(body, out_shape, specs, scratch=(), flops=1000000):
    return pl.pallas_call(
        body,
        out_shape=out_shape,
        in_specs=specs,
        out_specs=jax.tree.map(lambda _: VMEM, out_shape),
        scratch_shapes=list(scratch),
        compiler_params=pltpu.CompilerParams(vmem_limit_bytes=VMEM_LIMIT),
        cost_estimate=pl.CostEstimate(flops=flops, bytes_accessed=1000000, transcendentals=0),
    )


def lanes(shape):
    return lax.broadcasted_iota(jnp.int32, shape, 1)


def rotate(v, shift, axis):
    return pltpu.roll(v, shift % v.shape[axis], axis)


def weigh(sigma):
    return jnp.where(sigma > 0.0, EDGE / (4.0 + sigma), 0.0)


def prepare(cond_in, rhs_in, fraction_in, region_in, flags_in, rhs, sigma, first_iter, packed_out, cond, fraction, region, flags, sems):
    half = BX // 2
    copies = [[pltpu.make_async_copy(cond_in, cond, sems.at[0])], []]
    for i in range(2):
        part = pl.ds(i * half, half)
        copies[i].append(pltpu.make_async_copy(region_in.at[part], region.at[part], sems.at[1 + 4 * i]))
        for j, (source, target) in enumerate(((fraction_in, fraction), (flags_in, flags), (rhs_in, rhs))):
            copies[i].append(pltpu.make_async_copy(source.at[:, part], target.at[:, part], sems.at[2 + 4 * i + j]))
    for copy in copies[0] + copies[1]:
        copy.start()
    group = lanes((8, BZ)) // 8
    for x in range(BX):
        if x % half == 0:
            for copy in copies[x // half]:
                copy.wait()
        where = region[x]
        conductivity = jnp.full((BY, BZ), cond[0], jnp.float32)
        for number in range(1, 8):
            conductivity = jnp.where(where == number, cond[number], conductivity)
        packed = jnp.zeros((8, BZ), jnp.float32)
        for field in range(6):
            if field < 3:
                value = rhs[field, x]
            else:
                c = field - 3
                value = jnp.where(flags[c, x] == 0, conductivity * fraction[c, x], 0.0)
                sigma[c, x] = value
                first_iter[c, x] = weigh(value) * rhs[c, x]
            for tile in range(2):
                slot = field * 2 + tile
                moved = rotate(value[tile * 8 : tile * 8 + 8], LOW + 8 * slot, 1)
                packed = jnp.where(group == slot, moved, packed)
        packed_out[x] = packed


def send_y(
    ypar, zpar, zlast, rhs, sigma, first_iter, from_even, from_odd, from_last, first_out, second_out, packed
):
    below = (lanes((8, BZ)) % 8) < LOW
    odd = (lanes((4, BZ)) // 8) % 2
    below = below == (zpar[0] == 0)
    for x in range(BX):
        packed[x] = jnp.where(below, jnp.where(zpar[0] == 0, from_odd[0, x], from_odd[1, x]), jnp.where(zlast[0] == 0, from_even[x], from_last[x]))

    def fill(out, layout, side):
        for p in OWN:
            for c in range(3):
                (at, count), (at_sigma, both) = layout[p, c], layout[p, c + 3]
                inner = 0 if side == ABOVE else BY - both
                outer = both if side == ABOVE else BY - count
                out[at_sigma : at_sigma + both] = sigma[c, p - LOW, inner : inner + both]
                place = at if side == ABOVE else at + count - both
                out[place : place + both] = rhs[c, p - LOW, inner : inner + both]
                place = at + both if side == ABOVE else at
                out[place : place + count - both] = first_iter[c, p - LOW, outer : outer + count - both]
        start = 0 if side == ABOVE else 4
        for p in OWN[::2]:
            value = packed[p - LOW, start : start + 4]
            other = packed[p + 1 - LOW, start : start + 4]
            at = layout[p, "packed"]
            out[at : at + 4] = jnp.where(odd == 1 - side, value, rotate(other, 8 if side == ABOVE else -8, 1))

    @pl.when(ypar[0] == 0)
    def _():
        fill(first_out, Y_LOW, BELOW)
        fill(second_out, Y_HIGH, ABOVE)

    @pl.when(ypar[0] != 0)
    def _():
        fill(second_out, Y_LOW, BELOW)
        fill(first_out, Y_HIGH, ABOVE)


def own_edge(p, y_low, y_high):
    odd = (lanes((4, BZ)) // 8) % 2 == 1
    above = y_high[Y_HIGH[p, "packed"] : Y_HIGH[p, "packed"] + 4]
    below = y_low[Y_LOW[p, "packed"] : Y_LOW[p, "packed"] + 4]
    if (p - LOW) % 2:
        above, below = rotate(above, -8, 1), rotate(below, 8, 1)
    return jnp.where(odd, below, above)


def first_lanes(p, value):
    fields = [c for c in range(3) if plane_need(c, p) == 1]
    if not fields:
        return value
    field = lanes(value.shape) // 16
    chosen = (field >= fields[0]) & (field <= fields[-1])
    return jnp.where(chosen, weigh(rotate(value, -48, 1)) * value, value)


def send_x(ypar, rhs, sigma, first_iter, packed, first, second, up_out, down_out, y_low, y_high):
    even = ypar[0] == 0
    y_high[...] = jnp.where(even, first[1], second[1])
    y_low[...] = jnp.where(even, second[0], first[0])
    for out, layout, planes, step in (
        (up_out, X_LOW, range(LOW), BX),
        (down_out, X_HIGH, range(LOW + BX, EXT), -BX),
    ):
        for p in planes:
            own = p + step
            x = own - LOW
            at = layout[p, "packed"]
            out[at : at + 8] = first_lanes(p, packed[x])
            at = layout[p, "edge"]
            out[at : at + 4] = first_lanes(p, own_edge(own, y_low, y_high))
            for c in range(3):
                if plane_need(c, p) == 2:
                    at = layout[p, c]
                    out[at : at + BY] = rhs[c, x]
                    at = layout[p, c + 3]
                    out[at : at + BY] = sigma[c, x]
                elif plane_need(c, p) == 1:
                    at = layout[p, c]
                    out[at : at + BY] = first_iter[c, x]
                for side, source, have in ((BELOW, y_low, Y_LOW), (ABOVE, y_high, Y_HIGH)):
                    (at, count), (at_sigma, both) = layout[p, c, side], layout[p, c + 3, side]
                    (own_at, own_count), (own_sigma, own_both) = have[own, c], have[own, c + 3]

                    def rows(base, size, near, far):
                        return slice(base + near, base + far) if side == ABOVE else slice(base + size - far, base + size - near)

                    if both:
                        out[rows(at_sigma, both, 0, both)] = source[rows(own_sigma, own_both, 0, both)]
                        out[rows(at, count, 0, both)] = source[rows(own_at, own_count, 0, both)]
                    middle = min(max(both, own_both), count)
                    if both < middle:
                        out[rows(at, count, both, middle)] = (
                            weigh(source[rows(own_sigma, own_both, both, middle)])
                            * source[rows(own_at, own_count, both, middle)]
                        )
                    if middle < count:
                        out[rows(at, count, middle, count)] = source[rows(own_at, own_count, middle, count)]


def up_y(v):
    return rotate(v, -1, 0)


def down_y(v):
    return rotate(v, 1, 0)


def up_z(v):
    return rotate(v, -1, 1)


def down_z(v):
    return rotate(v, 1, 1)


def spread(p, main, tile, packed, edge, wide, weight, iterate):
    edge = jnp.concatenate([edge, rotate(edge, -8, 1)], axis=0)
    row = lax.broadcasted_iota(jnp.int32, (8, BZ), 0)

    def parts(field):
        at = LOW + 16 * field
        return (
            (slice(0, BY), slice(0, BZ), main(field)),
            (slice(BY, 24), slice(0, BZ), tile(field)),
            (slice(0, 8), slice(BZ, None), rotate(packed, -at, 1)),
            (slice(8, BY), slice(BZ, None), rotate(packed, -(at + 8), 1)),
            (slice(BY, 24), slice(BZ, None), rotate(edge, -at, 1)),
        )

    for c in range(3):
        need = plane_need(c, p)
        if need == 0:
            continue
        if need == 1:
            for rows, columns, value in parts(c):
                iterate(c, p)[rows, columns] = value
            continue
        (low_any, low_both), (high_any, high_both) = row_counts(c, p)
        single = ((row >= high_both) & (row < high_any)) | ((row >= 8 - low_any) & (row < 8 - low_both))
        for i, ((rows, columns, rhs), (_, _, sigma)) in enumerate(zip(parts(c), parts(3 + c))):
            w = weigh(sigma)
            u = w * rhs
            if i == 1 and (high_any > high_both or low_any > low_both):
                u = jnp.where(single, rhs, u)
            wide(c, p)[rows, columns] = rhs
            wide(3 + c, p)[rows, columns] = sigma
            weight(c, p)[rows, columns] = w
            iterate(c, p)[rows, columns] = u


def faces(u, p):
    u0, u1, u2 = u(0, p)[...], u(1, p)[...], u(2, p)[...]
    f0 = (up_y(u2) - u2) - (up_z(u1) - u1)
    f1 = (up_z(u0) - u0) - (u(2, p + 1)[...] - u2)
    f2 = (u(1, p + 1)[...] - u1) - (up_y(u0) - u0)
    return f0, f1, f2


def curl0(f):
    return (down_z(f[1]) - f[1]) - (down_y(f[2]) - f[2])


def curl1(f, prev):
    return (prev[2] - f[2]) - (down_z(f[0]) - f[0])


def curl2(f, prev):
    return (down_y(f[0]) - f[0]) - (prev[1] - f[1])


def update(c, p, k, wide, weight, iterate):
    u = iterate(c, p)[...]
    return u + weight(c, p)[...] * (wide(c, p)[...] - (k + wide(3 + c, p)[...] * u))


def smooth(planes, prev, wide, weight, iterate, second_iter):
    for p in planes:
        f = faces(iterate, p)
        for c, k in enumerate((curl0(f), curl1(f, prev), curl2(f, prev))):
            second_iter(c, p)[...] = update(c, p, k, wide, weight, iterate)
        prev = f
    return prev


def defect(c, p, k, wide, second_iter):
    return wide(c, p)[...] - (k + wide(3 + c, p)[...] * second_iter(c, p)[...])


def kept(c, p, value, wide):
    return jnp.where(wide(3 + c, p)[...] > 0.0, value, 0.0)


def gather_nodes(p, before, q0, q1, q2, nodal):
    d1, d2 = down_y(q1), down_z(q2)
    nodal(0, p)[...] = (before - q0) + (d1 - q1) + (d2 - q2)
    nodal(1, p)[...] = (before + q0) * 0.5
    nodal(2, p)[...] = (d1 + q1) * 0.5
    nodal(3, p)[...] = (d2 + q2) * 0.5


def restrict(planes, prev, before, wide, second_iter, nodal):
    for p in planes:
        f = faces(second_iter, p)
        q = [
            kept(c, p, defect(c, p, k, wide, second_iter), wide)
            for c, k in enumerate((curl0(f), curl1(f, prev), curl2(f, prev)))
        ]
        gather_nodes(p, before, *q, nodal)
        prev, before = f, q[0]
    return prev, before


def beside(c, p, nodal):
    b = nodal(c, p)[...]
    return (1.2 * NODE) * b + (NODE * NODE) * ((up_y(b) + down_y(b)) + (up_z(b) + down_z(b)))


def finish(p, n0, n0_next, n1, n1_next, n2, n3, second_iter, rhs, sigma):
    corrections = (
        (n0_next - n0) + (n1_next + n1) * 0.5,
        (up_y(n0) - n0) + (n2 + up_y(n2)) * 0.5,
        (up_z(n0) - n0) + (n3 + up_z(n3)) * 0.5,
    )
    return [
        jnp.where(
            sigma[c, p - LOW] > 0.0,
            second_iter(c, p)[0:BY, 0:BZ] + corrections[c][0:BY, 0:BZ],
            0.96 * rhs[c, p - LOW],
        )
        for c in range(3)
    ]


INNER = {"wide": OWN, "weight": OWN, "iterate": OWN, "second": OWN[1:-1], "nodal": OWN[2:-2]}
USED = {"wide": range(EXT), "weight": range(EXT), "iterate": range(EXT), "second": range(1, EXT - 1), "nodal": range(2, EXT - 2)}
OUTER = {name: [p for p in USED[name] if p not in INNER[name]] for name in USED}
INNER |= {"second_part": OWN[:1], "second_carry": OWN[-2:-1], "nodal_part": OWN[1:2], "nodal_carry": OWN[-3:-2], "beside": OWN[2:-2]}
FIELDS = {
    "wide": 6, "weight": 3, "iterate": 3, "second": 3, "nodal": 4,
    "second_part": 3, "second_carry": 2, "nodal_part": 3, "nodal_carry": 3, "beside": 4,
}
MIDDLE = OWN[3]


def plane_arrays(kind, inner, outer=None):
    at = {p: (inner, i) for i, p in enumerate(INNER[kind])}
    if outer is not None:
        at.update({p: (outer, i) for i, p in enumerate(OUTER[kind])})
    return lambda c, p: at[p][0].at[c, at[p][1]]


def stencil_inner(rhs, sigma, packed, y_low, y_high, middle, *arrays):
    wide, weight, iterate, second_iter, nodal, second_part, second_carry, nodal_part, nodal_carry, near = (
        plane_arrays(kind, ref) for kind, ref in zip(FIELDS, arrays)
    )
    for p in OWN:

        def main(field):
            return (rhs if field < 3 else sigma)[field % 3, p - LOW]

        def tile(field):
            target = wide(field, p)
            for ref, layout, below in ((y_low, Y_LOW, True), (y_high, Y_HIGH, False)):
                at, count = layout[p, field]
                start = 24 - count if below else BY
                target[start : start + count, 0:BZ] = ref[at : at + count]
            return target[BY:24, 0:BZ]

        spread(p, main, tile, packed[p - LOW], own_edge(p, y_low, y_high), wide, weight, iterate)

    p = OWN[0]
    prev = f = faces(iterate, p)
    k = (curl0(f), -f[2] - (down_z(f[0]) - f[0]), (down_y(f[0]) - f[0]) + f[1])
    for c in range(3):
        second_part(c, p)[...] = update(c, p, k[c], wide, weight, iterate)
    prev = smooth(INNER["second"], prev, wide, weight, iterate, second_iter)
    for i in range(2):
        second_carry(i, INNER["second"][-1])[...] = prev[1 + i]

    p = OWN[1]
    prev = f = faces(second_iter, p)
    before = kept(0, p, defect(0, p, curl0(f), wide, second_iter), wide)
    nodal_part(0, p)[...] = before
    nodal_part(1, p)[...] = defect(1, p, -f[2] - (down_z(f[0]) - f[0]), wide, second_iter)
    nodal_part(2, p)[...] = defect(2, p, (down_y(f[0]) - f[0]) + f[1], wide, second_iter)
    prev, before = restrict(INNER["nodal"], prev, before, wide, second_iter, nodal)
    for i, value in enumerate((prev[1], prev[2], before)):
        nodal_carry(i, INNER["nodal"][-1])[...] = value

    for p in INNER["beside"]:
        for c in range(4):
            near(c, p)[...] = beside(c, p, nodal)

    def node(c, p):
        return near(c, p)[...] + (NODE * NODE) * (nodal(c, p - 1)[...] + nodal(c, p + 1)[...])

    p = MIDDLE
    planes = finish(
        p, node(0, p), node(0, p + 1), node(1, p), node(1, p + 1), node(2, p), node(3, p), second_iter, rhs, sigma
    )
    for c in range(3):
        middle[c] = planes[c]


def stencil_outer(rhs, sigma, low, high, middle, *arrays):
    inner, out, outer = arrays[: len(FIELDS)], arrays[len(FIELDS)], arrays[len(FIELDS) + 1 :]
    wide, weight, iterate, second_iter, nodal = (plane_arrays(k, *refs) for k, refs in zip(FIELDS, zip(inner, outer)))
    second_part, second_carry, nodal_part, nodal_carry, near = (
        plane_arrays(kind, ref) for kind, ref in list(zip(FIELDS, inner))[5:]
    )
    upper = lax.broadcasted_iota(jnp.int32, (8, BZ), 0) < 4
    for p in OUTER["wide"]:
        ref, layout = (low, X_LOW) if p < LOW else (high, X_HIGH)

        def main(field):
            return ref[layout[p, field] : layout[p, field] + BY]

        def tile(field):
            (below, count), (above, _) = layout[p, field, BELOW], layout[p, field, ABOVE]
            return jnp.where(upper, ref[above : above + 8], ref[below + count - 8 : below + count])

        packed, edge = layout[p, "packed"], layout[p, "edge"]
        spread(p, main, tile, ref[packed : packed + 8], ref[edge : edge + 4], wide, weight, iterate)

    first, last = INNER["second"][0] - 1, INNER["second"][-1]
    prev = smooth(range(1, first), faces(iterate, 0), wide, weight, iterate, second_iter)
    second_iter(0, first)[...] = second_part(0, first)[...]
    second_iter(1, first)[...] = second_part(1, first)[...] - weight(1, first)[...] * prev[2]
    second_iter(2, first)[...] = second_part(2, first)[...] + weight(2, first)[...] * prev[1]
    prev = (None, second_carry(0, last)[...], second_carry(1, last)[...])
    smooth(range(last + 1, EXT - 1), prev, wide, weight, iterate, second_iter)

    first, last = INNER["nodal"][0] - 1, INNER["nodal"][-1]
    prev = faces(second_iter, 1)
    before = kept(0, 1, defect(0, 1, curl0(prev), wide, second_iter), wide)
    prev, before = restrict(range(2, first), prev, before, wide, second_iter, nodal)
    q1 = kept(1, first, nodal_part(1, first)[...] - prev[2], wide)
    q2 = kept(2, first, nodal_part(2, first)[...] + prev[1], wide)
    gather_nodes(first, before, nodal_part(0, first)[...], q1, q2, nodal)
    prev = (None, nodal_carry(0, last)[...], nodal_carry(1, last)[...])
    restrict(range(last + 1, EXT - 2), prev, nodal_carry(2, last)[...], wide, second_iter, nodal)

    def node(c, p):
        own = near(c, p)[...] if p in INNER["beside"] else beside(c, p, nodal)
        return own + (NODE * NODE) * (nodal(c, p - 1)[...] + nodal(c, p + 1)[...])

    n0, n1 = node(0, LOW), node(1, LOW)
    for p in OWN:
        n0_next, n1_next = node(0, p + 1), node(1, p + 1)
        if p == MIDDLE:
            planes = [middle[c] for c in range(3)]
        else:
            planes = finish(p, n0, n0_next, n1, n1_next, node(2, p), node(3, p), second_iter, rhs, sigma)
        for c in range(3):
            out[c, p - LOW] = planes[c]
        n0, n1 = n0_next, n1_next


def pairs(count):
    return (
        [[i, i + 1] for i in range(0, count, 2)],
        [[i, (i + 1) % count] for i in range(1, count, 2)],
    )


def gather(value, axis, groups):
    return lax.all_gather(value, axis, axis=0, tiled=False, axis_index_groups=groups)


def shift(value, axis, step):
    count = lax.axis_size(axis)
    return lax.ppermute(value, axis, [(i, (i + step) % count) for i in range(count)])


def on_device(rhs, conductivity, fraction, region, flags):
    f32 = functools.partial(jax.ShapeDtypeStruct, dtype=jnp.float32)
    ypar = (lax.axis_index("gy") & 1).astype(jnp.int32).reshape(1)
    zlast = (lax.axis_index("gz") >= lax.axis_size("gz") - 2).astype(jnp.int32).reshape(1)
    zpar = (lax.rem(lax.axis_index("gz"), 2)).astype(jnp.int32).reshape(1)

    block = f32((3, BX, BY, BZ))
    lane_block = f32((BX, 8, BZ))
    rhs, sigma, first_iter, packed = call(
        prepare,
        (block, block, block, lane_block),
        [HBM] * 5,
        scratch=(
            pltpu.SMEM((8,), jnp.float32),
            pltpu.VMEM((3, BX, BY, BZ), jnp.float32),
            pltpu.VMEM((BX, BY, BZ), jnp.int32),
            pltpu.VMEM((3, BX, BY, BZ), jnp.int32),
            pltpu.SemaphoreType.DMA((9,)),
        ),
    )(*(pltpu.with_memory_space_constraint(a, pltpu.HBM) for a in (conductivity, rhs, fraction, region, flags)))

    nz = lax.axis_size("gz")
    from_even = lax.ppermute(packed, "gz", [(i, i ^ 1) for i in range(nz - 2)])
    from_odd = gather(packed, "gz", pairs(nz)[1])
    from_last = lax.ppermute(packed, "gz", [(nz - 2, nz - 1), (nz - 1, nz - 2)])

    even_y, odd_y = pairs(lax.axis_size("gy"))
    payload = f32((Y_ROWS, BZ))
    to_first, to_second, packed = call(
        send_y, (payload, payload, lane_block), [SMEM] * 3 + [VMEM] * 6
    )(ypar, zpar, zlast, rhs, sigma, first_iter, from_even, from_odd, from_last)
    first = gather(to_first, "gy", even_y)
    second = gather(to_second, "gy", odd_y)

    up, down, y_low, y_high = call(
        send_x, (f32((X_LOW_ROWS, BZ)), f32((X_HIGH_ROWS, BZ)), payload, payload), [SMEM] + [VMEM] * 6
    )(ypar, rhs, sigma, first_iter, packed, first, second)
    low = shift(up, "gx", 1)
    high = shift(down, "gx", -1)

    inner = call(
        stencil_inner,
        (f32((3, BY, BZ)), *(f32((FIELDS[kind], len(INNER[kind]), 24, 2 * BZ)) for kind in FIELDS)),
        [VMEM] * 5,
        flops=20000000,
    )(rhs, sigma, packed, y_low, y_high)
    return call(
        stencil_outer,
        block,
        [VMEM] * (5 + len(FIELDS)),
        scratch=[pltpu.VMEM((FIELDS[kind], len(OUTER[kind]), 24, 2 * BZ), jnp.float32) for kind in OUTER],
    )(rhs, sigma, low, high, *inner)


def solution(mesh):
    return jax.shard_map(
        on_device,
        mesh=mesh,
        in_specs=(
            P(None, "gx", "gy", "gz"),
            P(),
            P(None, "gx", "gy", "gz"),
            P("gx", "gy", "gz"),
            P(None, "gx", "gy", "gz"),
        ),
        out_specs=P(None, "gx", "gy", "gz"),
        check_vma=False,
    )
```
